512 devices in a mesh: gx: 16 (over z_hi, y, core), gy: 32 (over z_lo, x).
Axes of the slice: x: 4, y: 4, z: 16 (z_hi: 2, z_lo: 8; z = z_hi * 8 + z_lo), core: 2. Of those that a mesh axis runs over, the one named last changes fastest.
Arguments:
- features: bfloat16 [16, 32, 128, 256], P('gx', 'gy'), may hold values from -6 to 6
- occupancy: int32 [16, 32, 128], P('gx', 'gy'), may hold values from 0 to 1, as said below
- coords: int32 [16, 32, 3, 128], P('gx', 'gy'), may hold values from 0 to 7, as said below
- norm_gains: float32 [2, 2, 256], replicated, may hold values from 0.1 to 1.9
- bias_tables: float32 [2, 3, 8, 15], replicated, may hold values from -4 to 4
- w_qkv: bfloat16 [2, 256, 768], replicated, may hold values from -0.375 to 0.375
- w_out: bfloat16 [2, 256, 256], replicated, may hold values from -0.375 to 0.375
- w_up: bfloat16 [2, 256, 1024], replicated, may hold values from -0.375 to 0.375
- w_down: bfloat16 [2, 1024, 256], replicated, may hold values from -0.1875 to 0.1875
- grad_out: bfloat16 [16, 32, 128, 256], P('gx', 'gy'), may hold values from -6 to 6
Outputs:
- out_points: bfloat16 [16, 32, 128, 256], P('gx', 'gy')
- grad_points: bfloat16 [16, 32, 128, 256], P('gx', 'gy')
- grad_tables: float32 [2, 3, 8, 15], replicated
The draws below stay inside these ranges and needn't reach their ends.
Inputs may be any that keep to these rules, and one draw needn't show every extreme that they name: `occupancy`: 1 marks an occupied slot. In each quarter of 32 slots of a window the occupied slots come first, and every quarter holds at least one. `coords`: the x coordinate of a slot of quarter (a, b) lies in [a * 4, (a + 1) * 4) and its y coordinate in [b * 4, (b + 1) * 4); z lies in [0, 8).
All inputs are finite; a program needn't handle non-finite values.
Results may differ from the reference program's by a relative error of at most 0.02.
Values may be sent and summed in bfloat16 or wider, within the bound.
No kernel may reach another device: no remote copies, remote signals or barrier semaphores. Data moves between devices by JAX's collectives and lax.ppermute only.
A program may use at most 64 MiB of HBM per device.

```python
from functools import partial
import jax
import jax.numpy as jnp
from jax import lax

C = 256
HEADS = 8
FF = 1024
SLOTS = 128
QUAD = 32
WS = 8
NREL = 15
NWX = 16
NWY = 32


def draw_occupancy(key, part):
    level_key, count_key = jax.random.split(key)
    levels = jax.random.randint(level_key, (NWX, NWY, 1), 0, 4)
    lower = levels * (QUAD // 4) + 1
    upper = jnp.minimum((levels + 2) * (QUAD // 4), QUAD) + 1
    counts = jax.random.randint(count_key, (NWX, NWY, 4), lower, upper)
    slot_rank = jnp.arange(QUAD, dtype=jnp.int32)
    filled = (slot_rank[None, None, None, :] < counts[..., None]).astype(jnp.int32)
    return filled.reshape(NWX, NWY, SLOTS)


def draw_coords(key, part):
    half_span = WS // 2
    slot_index = jnp.arange(SLOTS, dtype=jnp.int32)
    upper_x = slot_index // (2 * QUAD)
    upper_y = slot_index // QUAD % 2
    keys_three = jax.random.split(jax.random.fold_in(key, 7), 3)
    within_x = jax.random.randint(keys_three[0], (NWX, NWY, SLOTS), 0, half_span)
    within_y = jax.random.randint(keys_three[1], (NWX, NWY, SLOTS), 0, half_span)
    coord_z = jax.random.randint(keys_three[2], (NWX, NWY, SLOTS), 0, WS)
    coord_x = upper_x[None, None, :] * half_span + within_x
    coord_y = upper_y[None, None, :] * half_span + within_y
    return jnp.stack([coord_x, coord_y, coord_z], axis=2).astype(jnp.int32)


def level_of(own_key, extent, cuts, smallest, top_value):
    loudness, own = 1.0, jax.random.fold_in(own_key, 6)
    for dim, blocks in cuts:
        heights = jnp.exp(jax.random.uniform(jax.random.fold_in(own, dim), (blocks,), jnp.float32, smallest / len(cuts), top_value / len(cuts)))
        loudness = loudness * jnp.repeat(heights, extent[dim] // blocks).reshape([-1 if axis == dim else 1 for axis in range(len(extent))])
    return loudness


def scatter_about(own_key, dims, scale, reach, pieces=(), kind=jnp.bfloat16):
    values = scale * jax.random.normal(own_key, dims, jnp.float32)
    if pieces:
        values = values * level_of(own_key, dims, pieces, -0.22, 0.18)
    return jnp.clip(values, -reach, reach).astype(kind)


def setup_inputs(seed: int = 0) -> dict:
    seeds = jax.random.split(jax.random.key(seed), 11)
    features = scatter_about(seeds[0], (NWX, NWY, SLOTS, C), 1.0, 6.0, ((0, 16), (1, 32)))
    occupancy = draw_occupancy(jax.random.fold_in(seeds[10], 71), 0)
    coords = draw_coords(jax.random.fold_in(seeds[10], 71), 0)
    norm_gains = jnp.clip(1.0 + 0.18 * jax.random.normal(seeds[3], (2, 2, C), jnp.float32), 0.1, 1.9)
    bias_tables = scatter_about(seeds[4], (2, 3, HEADS, NREL), 1.0, 4.0, (), jnp.float32)
    w_qkv = scatter_about(seeds[5], (2, C, 3 * C), C ** -0.5, 0.375)
    w_out = scatter_about(seeds[6], (2, C, C), C ** -0.5, 0.375)
    w_up = scatter_about(seeds[7], (2, C, FF), C ** -0.5, 0.375)
    w_down = scatter_about(seeds[8], (2, FF, C), FF ** -0.5, 0.1875)
    grad_out = scatter_about(seeds[9], (NWX, NWY, SLOTS, C), 1.0, 6.0, ((0, 16), (1, 32)))
    return dict(features=features, occupancy=occupancy, coords=coords, norm_gains=norm_gains, bias_tables=bias_tables, w_qkv=w_qkv, w_out=w_out, w_up=w_up, w_down=w_down, grad_out=grad_out)


highest_precision = lax.Precision.HIGHEST
epsilon = 1e-05

def layer_norm(values, gain):
    mean_value = lax.optimization_barrier(jnp.mean(values, axis=-1, keepdims=True))
    centred = values - mean_value
    variance = lax.optimization_barrier(jnp.mean(centred * centred, axis=-1, keepdims=True))
    return centred * lax.rsqrt(variance + epsilon) * gain

def relative_bias(coords, bias_table):
    table_span = bias_table.shape[-1]
    window_span = (table_span + 1) // 2
    cell_index = jnp.arange(window_span, dtype=jnp.int32)
    offsets = cell_index[:, None] - cell_index[None, :] + window_span - 1
    selection_matrix = (offsets[:, :, None] == jnp.arange(table_span, dtype=jnp.int32)[None, None, :]).astype(jnp.float32)
    total = None
    for axis_index in range(3):
        indicator_matrix = (coords[axis_index][:, None] == cell_index[None, :]).astype(jnp.float32)
        banded_offset_matrix = jnp.einsum('hr,abr->hab', bias_table[axis_index], selection_matrix, precision=highest_precision)
        left_factor = jnp.einsum('dx,cxq->cdq', indicator_matrix, banded_offset_matrix, precision=highest_precision)
        axis_contribution_part = jnp.einsum('klu,tu->klt', left_factor, indicator_matrix, precision=highest_precision)
        total = axis_contribution_part if total is None else total + axis_contribution_part
    return total

def attend(queries, keys_part, values_part, bias_table, occupied, coords):
    head_size = queries.shape[-1]
    scores = jnp.einsum('qhd,khd->hqk', queries.astype(jnp.float32), keys_part.astype(jnp.float32), precision=highest_precision)
    scores = scores * head_size ** (-0.5) + relative_bias(coords, bias_table)
    scores = jnp.where(occupied[None, None, :] > 0, scores, -1e+30)
    weights_soft = jax.nn.softmax(scores, axis=-1).astype(jnp.bfloat16)
    mixed = jnp.einsum('hqk,khd->qhd', weights_soft.astype(jnp.float32), values_part.astype(jnp.float32), precision=highest_precision)
    return mixed.reshape(mixed.shape[0], -1).astype(jnp.bfloat16)

def swin_block(hidden, bias_table, occupied, coords, gains, weight_qkv, weight_out, up_weight_matrix, weight_down):
    slots, width = hidden.shape
    heads = bias_table.shape[1]
    core = jax.checkpoint(partial(attend, occupied=occupied, coords=coords))
    normed = layer_norm(hidden.astype(jnp.float32), gains[0]).astype(jnp.bfloat16)
    projected = jnp.dot(normed, weight_qkv, preferred_element_type=jnp.float32).astype(jnp.bfloat16)
    qkv_parts = projected.reshape(slots, 3, heads, width // heads)
    mixed = core(qkv_parts[:, 0], qkv_parts[:, 1], qkv_parts[:, 2], bias_table)
    middle = hidden.astype(jnp.float32) + jnp.dot(mixed, weight_out, preferred_element_type=jnp.float32)
    normed_two = layer_norm(middle, gains[1]).astype(jnp.bfloat16)
    expanded = jax.nn.gelu(jnp.dot(normed_two, up_weight_matrix, preferred_element_type=jnp.float32)).astype(jnp.bfloat16)
    return (middle + jnp.dot(expanded, weight_down, preferred_element_type=jnp.float32)).astype(jnp.bfloat16)

def roll_grid(array, shift_count):
    count_x, count_y = (array.shape[0], array.shape[1])
    trailing = array.shape[4:]
    quarter_grid = jnp.swapaxes(array, 1, 2).reshape((2 * count_x, 2 * count_y) + trailing)
    quarter_grid = jnp.roll(quarter_grid, (shift_count, shift_count), axis=(0, 1))
    return jnp.swapaxes(quarter_grid.reshape((count_x, 2, count_y, 2) + trailing), 1, 2)

def roll_points(points, shift_count):
    count_x, count_y, slots, width = points.shape
    tiles = points.reshape(count_x, count_y, 2, 2, slots // 4, width)
    return roll_grid(tiles, shift_count).reshape(points.shape)

def reference(features, occupancy, coords, norm_gains, bias_tables, w_qkv, w_out, w_up, w_down, grad_out):
    count_x, count_y, slots, width = features.shape
    quarter = slots // 4
    window_span = (bias_tables.shape[-1] + 1) // 2
    half_span = window_span // 2
    slot_meta = jnp.concatenate([occupancy[:, :, None, :], coords], axis=2)
    meta_tiles = jnp.moveaxis(slot_meta.reshape(count_x, count_y, 4, 2, 2, quarter), 2, -1)
    meta_tiles = jnp.moveaxis(roll_grid(meta_tiles, -1), -1, 2).reshape(count_x, count_y, 4, slots)
    shifted_coords = jnp.stack([(meta_tiles[:, :, 1] + half_span) % window_span, (meta_tiles[:, :, 2] + half_span) % window_span, meta_tiles[:, :, 3]], axis=2)
    occupied = occupancy.astype(jnp.float32)
    shifted_occupied = meta_tiles[:, :, 0].astype(jnp.float32)
    occupied_mask = occupancy.astype(jnp.bfloat16)[..., None]

    def apply_windows(points, bias_table, occupied_in, coords_in, block_index):

        def one_window(packed):
            return swin_block(packed[0], bias_table, packed[1], packed[2], norm_gains[block_index], w_qkv[block_index], w_out[block_index], w_up[block_index], w_down[block_index])
        per_window = lax.map(one_window, (points.reshape(-1, slots, width), occupied_in.reshape(-1, slots), coords_in.reshape(-1, 3, slots)))
        return per_window.reshape(points.shape)

    def run_blocks(points, tables):
        first_out = apply_windows(points, tables[0], occupied, coords, 0)
        second = apply_windows(roll_points(first_out, -1), tables[1], shifted_occupied, shifted_coords, 1)
        return roll_points(second, 1) * occupied_mask
    out_points, pullback = jax.vjp(run_blocks, features, bias_tables)
    grad_points, grad_tables = pullback(grad_out)
    return (out_points, grad_points, grad_tables)
```

```python
from functools import partial

import jax
import jax.numpy as jnp
from jax import lax
from jax.experimental import pallas as pl
from jax.experimental.pallas import tpu as pltpu
from jax.sharding import Mesh
from jax.sharding import PartitionSpec as P

INTERPRET = False
EPS = 1e-05
BF = jnp.bfloat16
F32 = jnp.float32
SLOTS, WIDTH, HEADS, HD, QUAD = 128, 256, 8, 32, 32
SPAN, PITCH = 8, 16
SCALE = HD ** (-0.5)
MASKED = -1e30
VMEM_LIMIT = 24 * 1024 * 1024


def mm(a, b):
    return lax.dot_general(a, b, (((1,), (0,)), ((), ())), preferred_element_type=F32)


def mm_t(a, b):
    return lax.dot_general(a, b, (((1,), (1,)), ((), ())), preferred_element_type=F32)


def iota(shape, axis):
    return lax.broadcasted_iota(jnp.int32, shape, axis)


def normalise(values):
    centred = values - jnp.mean(values, axis=-1, keepdims=True)
    inv = lax.rsqrt(jnp.mean(centred * centred, axis=-1, keepdims=True) + EPS)
    return centred * inv, inv


def normalise_back(cot, unit, inv):
    return inv * (
        cot
        - jnp.mean(cot, axis=-1, keepdims=True)
        - unit * jnp.mean(cot * unit, axis=-1, keepdims=True)
    )


def cells(coords, mirrored):
    row = iota((PITCH, SLOTS), 0)
    if mirrored:
        row = SPAN - 1 - row
    return jnp.concatenate(
        [(coords[e : e + 1] == row).astype(F32) for e in range(3)], axis=0
    )


def slot_matrices(coords, occupied):
    mirrored = cells(coords, True)
    first_row = iota((PITCH, SLOTS), 0) == 0
    ones = jnp.where(first_row, 1.0, 0.0)
    mask = jnp.where(first_row & (occupied <= 0), MASKED, 0.0)
    blank = jnp.zeros((PITCH, SLOTS), F32)
    query = jnp.concatenate([mirrored, ones, blank, blank, blank, blank], axis=0)
    key = jnp.concatenate([mirrored, mirrored, mask, blank], axis=0)
    return jnp.transpose(query).astype(BF), jnp.transpose(key).astype(BF)


def table_matrix(table):
    lane = iota((SPAN, 128), 1)
    wide = []
    for e in range(3):
        row = jnp.concatenate(
            [table[e] * (1.0 / SCALE), jnp.zeros((HEADS, 128 - table.shape[-1]), F32)], axis=1
        )
        start = e * PITCH - (SPAN - 1)
        wide.append(
            pltpu.roll(row, start % 128, 1) + pltpu.roll(row, (start + 3 * PITCH) % 128, 1)
        )
    columns = []
    for h in range(HEADS):
        rows = []
        for e in range(3):
            value = pltpu.roll(
                jnp.broadcast_to(wide[e][h : h + 1], (SPAN, 128)), 0, 1, stride=1, stride_axis=0
            )
            high = value.astype(BF).astype(F32)
            value = jnp.where(lane < 3 * PITCH, high, value - high)
            base = lane % (3 * PITCH) - e * PITCH
            keep = (base >= 0) & (base < SPAN) & (lane < 6 * PITCH)
            rows += [jnp.where(keep, value, 0.0), jnp.zeros((SPAN, 128), F32)]
        one = (iota((PITCH, 128), 0) == 0) & (iota((PITCH, 128), 1) == 6 * PITCH)
        rows += [jnp.where(one, 1.0, 0.0), jnp.zeros((128 - 4 * PITCH, 128), F32)]
        columns.append(jnp.concatenate(rows, axis=0))
    return jnp.concatenate(columns, axis=1).astype(BF)


def spread(group):
    head = iota(group.shape, 1) // HD
    return jnp.concatenate(
        [jnp.where(head == j, group, jnp.zeros_like(group)) for j in range(4)], axis=0
    )


def side_by_side(stack):
    return jnp.concatenate([stack[j * SLOTS : (j + 1) * SLOTS] for j in range(4)], axis=1)


def gelu_parts(v):
    c = 0.7978845608028654
    t = jnp.tanh(c * (v + 0.044715 * (v * v * v)))
    return 0.5 * v * (1.0 + t), t


def gelu_slope(v):
    c = 0.7978845608028654
    t = jnp.tanh(c * (v + 0.044715 * (v * v * v)))
    return 0.5 * (1.0 + t) + 0.5 * v * (1.0 - t * t) * c * (1.0 + 3 * 0.044715 * (v * v))


def block_forward(hidden, gains, coords, occupied, table, w_qkv, w_out, w_up, w_down):
    unit, _ = normalise(hidden)
    projected = mm((unit * gains[0:1]).astype(BF), w_qkv[...]).astype(BF)
    query_side, key_side = slot_matrices(coords, occupied)
    bias_left = mm(query_side, table_matrix(table)).astype(BF)
    probs, mixed = [], []
    for g in range(2):
        q = projected[:, 128 * g : 128 * g + 128]
        k = projected[:, 256 + 128 * g : 256 + 128 * g + 128]
        v = projected[:, 512 + 128 * g : 512 + 128 * g + 128]
        lefts = jnp.concatenate(
            [bias_left[:, 128 * h : 128 * h + 128] for h in range(4 * g, 4 * g + 4)], axis=0
        )
        scores = mm_t(
            jnp.concatenate([spread(q), lefts], axis=1), jnp.concatenate([k, key_side], axis=1)
        )
        top = jnp.max(scores, axis=-1, keepdims=True)
        weights = jnp.exp((scores - top) * SCALE)
        soft = (weights * (1.0 / jnp.sum(weights, axis=-1, keepdims=True))).astype(BF)
        probs.append(soft)
        mixed.append(mm(side_by_side(soft), spread(v)))
    middle = hidden + mm(jnp.concatenate(mixed, axis=1).astype(BF), w_out[...])
    unit_two, _ = normalise(middle)
    up = mm((unit_two * gains[1:2]).astype(BF), w_up[...])
    expanded, _ = gelu_parts(up)
    out = middle + mm(expanded.astype(BF), w_down[...])
    return out.astype(BF), (projected, probs, middle, up)


def block_backward(cot, hidden, gains, coords, saved, w_qkv, w_out, w_up, w_down):
    projected, probs, middle, up = saved
    unit_two, inv_two = normalise(middle)
    cot_up = mm_t(cot, w_down[...]) * gelu_slope(up)
    cot_two = mm_t(cot_up.astype(BF), w_up[...]) * gains[1:2]
    cot_middle = cot.astype(F32) + normalise_back(cot_two, unit_two, inv_two)
    cot_mixed = mm_t(cot_middle.astype(BF), w_out[...]).astype(BF)
    cells_t = cells(coords, False).astype(BF)
    blank = jnp.zeros((SLOTS - 3 * PITCH, SLOTS), F32)
    cells_key = jnp.transpose(jnp.concatenate([cells(coords, True), blank], axis=0)).astype(BF)
    cot_q, cot_k, cot_v, pair_sums = [], [], [], []
    for g in range(2):
        q = projected[:, 128 * g : 128 * g + 128]
        k = projected[:, 256 + 128 * g : 256 + 128 * g + 128]
        v = projected[:, 512 + 128 * g : 512 + 128 * g + 128]
        dm = cot_mixed[:, 128 * g : 128 * g + 128]
        q_t = jnp.transpose(q.astype(F32)).astype(BF)
        dm_t = jnp.transpose(dm.astype(F32)).astype(BF)
        soft = probs[g]
        cot_soft = mm_t(spread(dm), v)
        weighted = soft.astype(F32) * cot_soft
        total = jnp.sum(weighted, axis=-1, keepdims=True)
        cot_scores = (weighted - soft.astype(F32) * total).astype(BF)
        cot_q.append(mm(side_by_side(cot_scores), spread(k)) * SCALE)
        k_rows, v_rows = [], []
        for j in range(4):
            rows = slice(j * SLOTS, (j + 1) * SLOTS)
            lanes = slice(j * HD, (j + 1) * HD)
            both = mm(jnp.concatenate([q_t[lanes], cells_t], axis=0), cot_scores[rows])
            k_rows.append(both[:HD])
            pair_sums.append(both[HD:])
            v_rows.append(mm(dm_t[lanes], soft[rows]))
        cot_k.append(jnp.transpose(jnp.concatenate(k_rows, axis=0)) * SCALE)
        cot_v.append(jnp.transpose(jnp.concatenate(v_rows, axis=0)))
    cot_projected = jnp.concatenate(cot_q + cot_k + cot_v, axis=1).astype(BF)
    cot_normed = mm_t(cot_projected, w_qkv[...]) * gains[0:1]
    unit, inv = normalise(hidden)
    cot_hidden = cot_middle + normalise_back(cot_normed, unit, inv)
    pairs = mm(jnp.concatenate(pair_sums, axis=0).astype(BF), cells_key)
    lane = iota((SPAN, 128), 1)
    tables = []
    for h in range(HEADS):
        per_axis = [
            pairs[(3 * h + e) * PITCH : (3 * h + e) * PITCH + SPAN] for e in range(3)
        ]
        value = jnp.where(lane < PITCH, per_axis[0], jnp.where(lane < 2 * PITCH, per_axis[1], per_axis[2]))
        value = jnp.where(lane < 3 * PITCH, value, 0.0)
        value = pltpu.roll(value, 0, 1, stride=1, stride_axis=0)
        tables.append(jnp.sum(value, axis=0, keepdims=True))
    return cot_hidden.astype(BF), jnp.concatenate(tables, axis=0)


def first_kernel(
    features, occupancy, coords, gains, tables, w_qkv, w_out, w_up, w_down, grad_out,
    own, to_y, to_x, to_xy, projected, probs, middle, up,
):
    occupied = occupancy[...]
    place = coords[...]
    out, saved = block_forward(
        features[...].astype(F32), gains[0], place, occupied, tables[0],
        w_qkv.at[0], w_out.at[0], w_up.at[0], w_down.at[0],
    )
    projected[...] = saved[0]
    probs[0] = saved[1][0]
    probs[1] = saved[1][1]
    middle[...] = saved[2]
    up[...] = saved[3]
    column = jnp.transpose(jnp.broadcast_to(occupied.astype(F32), (SLOTS, SLOTS)))
    grad = grad_out[...] * jnp.concatenate([column, column], axis=1).astype(BF)
    meta = jnp.concatenate([occupied, place, jnp.zeros((4, SLOTS), jnp.int32)], axis=0).astype(F32)
    meta = jnp.concatenate([meta, jnp.zeros((8, SLOTS), F32)], axis=0)
    meta = jnp.concatenate([meta, jnp.zeros((16, SLOTS), F32)], axis=1).astype(BF)
    for quarter, target in ((3, own), (2, to_y), (1, to_x), (0, to_xy)):
        rows = slice(quarter * QUAD, (quarter + 1) * QUAD)
        target[0:QUAD] = out[rows]
        target[QUAD : 2 * QUAD] = grad[rows]
        target[2 * QUAD : 2 * QUAD + 16] = meta


def second_kernel(
    own, from_y, from_x, from_xy, gains, tables, w_qkv, w_out, w_up, w_down,
    back_own, back_y, back_x, back_xy, table_cot,
):
    parts = (own, from_y, from_x, from_xy)
    hidden = jnp.concatenate([part[0:QUAD] for part in parts], axis=0).astype(F32)
    grad = jnp.concatenate([part[QUAD : 2 * QUAD] for part in parts], axis=0)
    quarter = iota((8, SLOTS), 1) // QUAD
    meta = jnp.zeros((8, SLOTS), F32)
    for position, part in enumerate(parts):
        rows = part[2 * QUAD : 2 * QUAD + 16].astype(F32)[0:8, 0:SLOTS]
        rows = pltpu.roll(rows, (2 * position - 3) * QUAD % SLOTS, 1)
        meta = jnp.where(quarter == position, rows, meta)
    meta = meta.astype(jnp.int32)
    half = SPAN // 2
    occupied = meta[0:1]
    place = jnp.concatenate(
        [(meta[1:2] + half) % SPAN, (meta[2:3] + half) % SPAN, meta[3:4]], axis=0
    )
    weights = (w_qkv.at[1], w_out.at[1], w_up.at[1], w_down.at[1])
    out, saved = block_forward(hidden, gains[1], place, occupied, tables[1], *weights)
    cot, table_cot[...] = block_backward(grad, hidden, gains[1], place, saved, *weights)
    for position, target in enumerate((back_own, back_y, back_x, back_xy)):
        rows = slice(position * QUAD, (position + 1) * QUAD)
        target[0:QUAD] = out[rows]
        target[QUAD : 2 * QUAD] = cot[rows]


def third_kernel(
    from_xy, from_x, from_y, own, features, occupancy, coords, gains, w_qkv, w_out, w_up, w_down,
    projected, probs, middle, up, table_cot,
    out_points, grad_points, tables_out,
):
    occupied = occupancy[...]
    parts = (from_xy, from_x, from_y, own)
    second = jnp.concatenate([part[0:QUAD] for part in parts], axis=0)
    cot = jnp.concatenate([part[QUAD : 2 * QUAD] for part in parts], axis=0)
    column = jnp.transpose(jnp.broadcast_to(occupied.astype(F32), (SLOTS, SLOTS)))
    out_points[...] = second * jnp.concatenate([column, column], axis=1).astype(BF)
    saved = (projected[...], (probs[0], probs[1]), middle[...], up[...])
    grad_points[...], table = block_backward(
        cot, features[...].astype(F32), gains[0], coords[...], saved,
        w_qkv.at[0], w_out.at[0], w_up.at[0], w_down.at[0],
    )
    both = table + pltpu.roll(table_cot[...], 3 * PITCH, 1)
    for i in range(tables_out.shape[0]):
        tables_out[i] = both


def unpack_kernel(parts, out):
    total = parts[0]
    for i in range(1, parts.shape[0]):
        total = total + parts[i]
    for k in range(2):
        for e in range(3):
            start = (3 * k + e) * PITCH
            moved = total if start == 0 else pltpu.roll(total, 128 - start, 1)
            out[k, e] = moved[:, : out.shape[-1]]


def call(kernel, shapes, *args):
    return pl.pallas_call(
        kernel,
        out_shape=[jax.ShapeDtypeStruct(s, d) for s, d in shapes],
        compiler_params=pltpu.CompilerParams(vmem_limit_bytes=VMEM_LIMIT),
        interpret=INTERPRET,
    )(*args)


def shift(value, axes, steps):
    sizes = [lax.axis_size(a) for a in axes]
    count = 1
    for n in sizes:
        count *= n
    pairs = []
    for source in range(count):
        rest, target, stride = source, 0, 1
        for n, t in zip(reversed(sizes), reversed(steps)):
            target += (rest % n + t) % n * stride
            rest //= n
            stride *= n
        pairs.append((source, target))
    return lax.ppermute(value, axes, pairs)


def on_device(
    gx, gy, phases,
    features, occupancy, coords, norm_gains, bias_tables, w_qkv, w_out, w_up, w_down, grad_out,
):
    size_x = lax.axis_size(gx)
    size_y = lax.axis_size(gy)

    def move(value, step_x, step_y):
        pairs = []
        for i in range(size_x):
            for j in range(size_y):
                target = (i + step_x) % size_x * size_y + (j + step_y) % size_y
                pairs.append((i * size_y + j, target))
        return lax.ppermute(value, gx + gy, pairs)

    points, occupied, place = features[0, 0], occupancy[0], coords[0, 0]
    weights = (w_qkv, w_out, w_up, w_down)
    width_ff = w_up.shape[-1]
    packet = ((2 * QUAD + 16, WIDTH), BF)
    reply = ((2 * QUAD, WIDTH), BF)
    own, to_y, to_x, to_xy, *saved = call(
        first_kernel,
        [packet] * 4
        + [((SLOTS, 3 * WIDTH), BF), ((2, 4 * SLOTS, SLOTS), BF), ((SLOTS, WIDTH), F32), ((SLOTS, width_ff), F32)],
        points, occupied, place, norm_gains, bias_tables, *weights, grad_out[0, 0],
    )
    from_y, from_x, from_xy = move(to_y, 0, -1), move(to_x, -1, 0), move(to_xy, -1, -1)
    back_own, back_y, back_x, back_xy, table_cot = call(
        second_kernel,
        [reply] * 4 + [((HEADS, 128), F32)],
        own, from_y, from_x, from_xy, norm_gains, bias_tables, *weights,
    )
    home_y, home_x, home_xy = move(back_y, 0, 1), move(back_x, 1, 0), move(back_xy, 1, 1)
    first = lax.axis_size(phases[0])
    out_points, grad_points, tables = call(
        third_kernel,
        [((SLOTS, WIDTH), BF), ((SLOTS, WIDTH), BF), ((first, HEADS, 128), F32)],
        home_xy, home_x, home_y, back_own, points, occupied, place, norm_gains, *weights,
        *saved, table_cot,
    )
    for phase, after in zip(phases, phases[1:] + (None,)):
        tables = lax.all_to_all(tables, phase, 0, 0)
        if after is not None:
            tables = jnp.broadcast_to(
                jnp.sum(tables, axis=0)[None], (lax.axis_size(after), HEADS, 128)
            )
    (grad_tables,) = call(unpack_kernel, [(bias_tables.shape, F32)], tables)
    return out_points[None, None], grad_points[None, None], grad_tables


def solution(mesh):
    shape = tuple(mesh.shape[a] for a in ("gx", "gy"))
    if shape == (16, 32):
        fine = Mesh(mesh.devices.reshape(2, 4, 2, 8, 4), ("zh", "y", "c", "zl", "x"))
        gx, gy = ("zh", "y", "c"), ("zl", "x")
        phases = (("y", "c", "x"), ("zh", "zl"))
    else:
        fine = Mesh(mesh.devices, ("gx", "gy"))
        gx, gy, phases = ("gx",), ("gy",), (("gx",), ("gy",))
    grid = P(gx, gy, None, None)
    return jax.shard_map(
        partial(on_device, gx, gy, phases),
        mesh=fine,
        in_specs=(grid, P(gx, gy, None), grid, P(), P(), P(), P(), P(), P(), grid),
        out_specs=(grid, grid, P()),
        check_vma=False,
    )
```

```python
from functools import partial

import jax
import jax.numpy as jnp
from jax import lax
from jax.experimental import pallas as pl
from jax.experimental.pallas import tpu as pltpu
from jax.sharding import Mesh
from jax.sharding import PartitionSpec as P

INTERPRET = False
EPS = 1e-05
BF = jnp.bfloat16
F32 = jnp.float32
SLOTS, WIDTH, HEADS, HD, QUAD = 128, 256, 8, 32, 32
SPAN, PITCH = 8, 16
SCALE = HD ** (-0.5)
MASKED = -1e30
VMEM_LIMIT = 24 * 1024 * 1024


def mm(a, b):
    return lax.dot_general(a, b, (((1,), (0,)), ((), ())), preferred_element_type=F32)


def mm_t(a, b):
    return lax.dot_general(a, b, (((1,), (1,)), ((), ())), preferred_element_type=F32)


def mm_left(a, b):
    return lax.dot_general(a, b, (((0,), (0,)), ((), ())), preferred_element_type=F32)


def iota(shape, axis):
    return lax.broadcasted_iota(jnp.int32, shape, axis)


def normalise(values):
    centred = values - jnp.mean(values, axis=-1, keepdims=True)
    inv = lax.rsqrt(jnp.mean(centred * centred, axis=-1, keepdims=True) + EPS)
    return centred * inv, inv


def normalise_back(cot, unit, inv):
    return inv * (
        cot
        - jnp.mean(cot, axis=-1, keepdims=True)
        - unit * jnp.mean(cot * unit, axis=-1, keepdims=True)
    )


def cells(coords, mirrored):
    row = iota((PITCH, SLOTS), 0)
    if mirrored:
        row = SPAN - 1 - row
    return jnp.concatenate(
        [(coords[e : e + 1] == row).astype(F32) for e in range(3)], axis=0
    )


def query_cells(coords):
    ones = jnp.where(iota((PITCH, SLOTS), 0) == 0, 1.0, 0.0)
    return jnp.concatenate(
        [cells(coords, True), ones, jnp.zeros((SLOTS - 4 * PITCH, SLOTS), F32)], axis=0
    )


def key_cells(coords, occupied):
    mirrored = cells(coords, True)
    mask = jnp.where((iota((PITCH, SLOTS), 0) == 0) & (occupied <= 0), MASKED, 0.0)
    return jnp.concatenate([mirrored, mirrored, mask, jnp.zeros((PITCH, SLOTS), F32)], axis=0)


def table_matrix(table):
    lane = iota((SPAN, 128), 1)
    wide = []
    for e in range(3):
        row = jnp.concatenate(
            [table[e] * (1.0 / SCALE), jnp.zeros((HEADS, 128 - table.shape[-1]), F32)], axis=1
        )
        start = e * PITCH - (SPAN - 1)
        wide.append(
            pltpu.roll(row, start % 128, 1) + pltpu.roll(row, (start + 3 * PITCH) % 128, 1)
        )
    columns = []
    for h in range(HEADS):
        rows = []
        for e in range(3):
            value = pltpu.roll(
                jnp.broadcast_to(wide[e][h : h + 1], (SPAN, 128)), 0, 1, stride=1, stride_axis=0
            )
            high = value.astype(BF).astype(F32)
            value = jnp.where(lane < 3 * PITCH, high, value - high)
            base = lane % (3 * PITCH) - e * PITCH
            keep = (base >= 0) & (base < SPAN) & (lane < 6 * PITCH)
            rows += [jnp.where(keep, value, 0.0), jnp.zeros((SPAN, 128), F32)]
        one = (iota((PITCH, 128), 0) == 0) & (iota((PITCH, 128), 1) == 6 * PITCH)
        rows += [jnp.where(one, 1.0, 0.0), jnp.zeros((128 - 4 * PITCH, 128), F32)]
        columns.append(jnp.concatenate(rows, axis=0))
    return jnp.concatenate(columns, axis=1).astype(BF)


def spread(group):
    head = iota(group.shape, 1) // HD
    return jnp.concatenate(
        [jnp.where(head == j, group, jnp.zeros_like(group)) for j in range(4)], axis=0
    )


def side_by_side(stack):
    return jnp.concatenate([stack[j * SLOTS : (j + 1) * SLOTS] for j in range(4)], axis=1)


def softmax(scores):
    weights = jnp.exp((scores - jnp.max(scores, axis=-1, keepdims=True)) * SCALE)
    return (weights * (1.0 / jnp.sum(weights, axis=-1, keepdims=True))).astype(BF)


def gelu_parts(v):
    c = 0.7978845608028654
    t = jnp.tanh(c * (v + 0.044715 * (v * v * v)))
    return 0.5 * v * (1.0 + t), t


def gelu_slope(v):
    c = 0.7978845608028654
    t = jnp.tanh(c * (v + 0.044715 * (v * v * v)))
    return 0.5 * (1.0 + t) + 0.5 * v * (1.0 - t * t) * c * (1.0 + 3 * 0.044715 * (v * v))


def block_forward(hidden, gains, coords, occupied, table, w_qkv, w_out, w_up, w_down):
    unit, _ = normalise(hidden)
    projected = mm((unit * gains[0:1]).astype(BF), w_qkv[...]).astype(BF)
    query_side = jnp.transpose(query_cells(coords)).astype(BF)
    key_side = jnp.transpose(key_cells(coords, occupied)).astype(BF)
    bias_left = mm(query_side, table_matrix(table)).astype(BF)
    probs, mixed = [], []
    for g in range(2):
        q = projected[:, 128 * g : 128 * g + 128]
        k = projected[:, 256 + 128 * g : 256 + 128 * g + 128]
        v = projected[:, 512 + 128 * g : 512 + 128 * g + 128]
        lefts = jnp.concatenate(
            [bias_left[:, 128 * h : 128 * h + 128] for h in range(4 * g, 4 * g + 4)], axis=0
        )
        scores = mm_t(
            jnp.concatenate([spread(q), lefts], axis=1), jnp.concatenate([k, key_side], axis=1)
        )
        soft = softmax(scores)
        probs.append(soft)
        mixed.append(mm(side_by_side(soft), spread(v)))
    middle = hidden + mm(jnp.concatenate(mixed, axis=1).astype(BF), w_out[...])
    unit_two, _ = normalise(middle)
    up = mm((unit_two * gains[1:2]).astype(BF), w_up[...])
    expanded, _ = gelu_parts(up)
    out = middle + mm(expanded.astype(BF), w_down[...])
    return out.astype(BF), (projected, probs, middle, up)


def feed_forward_back(cot, gains, middle, up, w_out, w_up, w_down):
    unit, inv = normalise(middle)
    cot_up = mm_t(cot, w_down[...]) * gelu_slope(up)
    cot_two = mm_t(cot_up.astype(BF), w_up[...]) * gains[1:2]
    cot_middle = cot.astype(F32) + normalise_back(cot_two, unit, inv)
    return cot_middle, mm_t(cot_middle.astype(BF), w_out[...]).astype(BF)


def table_sums(per_head):
    lane = iota((SPAN, 128), 1)
    tables = []
    for blocks in per_head:
        value = jnp.where(lane < PITCH, blocks[0], jnp.where(lane < 2 * PITCH, blocks[1], blocks[2]))
        value = jnp.where(lane < 3 * PITCH, value, 0.0)
        value = pltpu.roll(value, 0, 1, stride=1, stride_axis=0)
        tables.append(jnp.sum(value, axis=0, keepdims=True))
    return jnp.concatenate(tables, axis=0)


def block_backward(cot, hidden, gains, coords, saved, w_qkv, w_out, w_up, w_down):
    projected, probs, middle, up = saved
    cot_middle, cot_mixed = feed_forward_back(cot, gains, middle, up, w_out, w_up, w_down)
    cells_t = cells(coords, False).astype(BF)
    blank = jnp.zeros((SLOTS - 3 * PITCH, SLOTS), F32)
    cells_key = jnp.transpose(jnp.concatenate([cells(coords, True), blank], axis=0)).astype(BF)
    cot_q, cot_k, cot_v, pair_sums = [], [], [], []
    for g in range(2):
        q = projected[:, 128 * g : 128 * g + 128]
        k = projected[:, 256 + 128 * g : 256 + 128 * g + 128]
        v = projected[:, 512 + 128 * g : 512 + 128 * g + 128]
        dm = cot_mixed[:, 128 * g : 128 * g + 128]
        q_t = jnp.transpose(q.astype(F32)).astype(BF)
        dm_t = jnp.transpose(dm.astype(F32)).astype(BF)
        soft = probs[g]
        cot_soft = mm_t(spread(dm), v)
        weighted = soft.astype(F32) * cot_soft
        total = jnp.sum(weighted, axis=-1, keepdims=True)
        cot_scores = (weighted - soft.astype(F32) * total).astype(BF)
        cot_q.append(mm(side_by_side(cot_scores), spread(k)) * SCALE)
        k_rows, v_rows = [], []
        for j in range(4):
            rows = slice(j * SLOTS, (j + 1) * SLOTS)
            lanes = slice(j * HD, (j + 1) * HD)
            both = mm(jnp.concatenate([q_t[lanes], cells_t], axis=0), cot_scores[rows])
            k_rows.append(both[:HD])
            pair_sums.append(both[HD:])
            v_rows.append(mm(dm_t[lanes], soft[rows]))
        cot_k.append(jnp.transpose(jnp.concatenate(k_rows, axis=0)) * SCALE)
        cot_v.append(jnp.transpose(jnp.concatenate(v_rows, axis=0)))
    cot_projected = jnp.concatenate(cot_q + cot_k + cot_v, axis=1).astype(BF)
    cot_normed = mm_t(cot_projected, w_qkv[...]) * gains[0:1]
    unit, inv = normalise(hidden)
    cot_hidden = cot_middle + normalise_back(cot_normed, unit, inv)
    pairs = mm(jnp.concatenate(pair_sums, axis=0).astype(BF), cells_key)
    per_head = [
        [pairs[(3 * h + e) * PITCH : (3 * h + e) * PITCH + SPAN] for e in range(3)]
        for h in range(HEADS)
    ]
    return cot_hidden.astype(BF), table_sums(per_head)


def head_lanes(stack):
    rows = stack.shape[0] // 4
    head = iota((rows, 128), 1) // HD
    out = jnp.zeros((rows, 128), stack.dtype)
    for j in range(4):
        out = jnp.where(head == j, stack[j * rows : (j + 1) * rows], out)
    return out


def halo_forward(points, places, occupieds, place, gains, table, w_qkv, w_out, w_up, w_down):
    unit, inv = normalise(points)
    normed = (unit * gains[0:1]).astype(BF)
    key_value = mm(normed, w_qkv[:, WIDTH:]).astype(BF)
    quarters = [slice(p * SLOTS + (3 - p) * QUAD, p * SLOTS + (4 - p) * QUAD) for p in range(4)]
    query = mm(jnp.concatenate([normed[r] for r in quarters], axis=0), w_qkv[:, :WIDTH]).astype(BF)
    hidden = jnp.concatenate([points[r] for r in quarters], axis=0)
    query_side = jnp.transpose(query_cells(place)).astype(BF)
    bias_left = mm(query_side, table_matrix(table)).astype(BF)
    probs, mixed, key_sides = {}, [], []
    for p in range(4):
        key_side = jnp.transpose(key_cells(places[p], occupieds[p])).astype(BF)
        key_sides.append(key_side)
        rows, window = slice(p * QUAD, (p + 1) * QUAD), slice(p * SLOTS, (p + 1) * SLOTS)
        groups = []
        for g in range(2):
            lanes = slice(128 * g, 128 * g + 128)
            k = key_value[window, 128 * g : 128 * g + 128]
            v = key_value[window, WIDTH + 128 * g : WIDTH + 128 * g + 128]
            lefts = jnp.concatenate(
                [bias_left[rows, 128 * h : 128 * h + 128] for h in range(4 * g, 4 * g + 4)], axis=0
            )
            scores = mm_t(
                jnp.concatenate([spread(query[rows, lanes]), lefts], axis=1),
                jnp.concatenate([k, key_side], axis=1),
            )
            probs[p, g] = softmax(scores)
            groups.append(head_lanes(mm(probs[p, g], v)))
        mixed.append(jnp.concatenate(groups, axis=1))
    middle = hidden + mm(jnp.concatenate(mixed, axis=0).astype(BF), w_out[...])
    unit_two, _ = normalise(middle)
    up = mm((unit_two * gains[1:2]).astype(BF), w_up[...])
    expanded, _ = gelu_parts(up)
    out = middle + mm(expanded.astype(BF), w_down[...])
    return out.astype(BF), (unit, inv, query, key_value, probs, key_sides, middle, up)


def halo_backward(cot, place, gains, saved, w_qkv, w_out, w_up, w_down):
    unit, inv, query, key_value, probs, key_sides, middle, up = saved
    cot_middle, cot_mixed = feed_forward_back(cot, gains, middle, up, w_out, w_up, w_down)
    cot_query, cot_windows, pair_rows = [], [], []
    for p in range(4):
        rows, window = slice(p * QUAD, (p + 1) * QUAD), slice(p * SLOTS, (p + 1) * SLOTS)
        cot_q, cot_k, cot_v, pairs = [], [], [], []
        for g in range(2):
            lanes = slice(128 * g, 128 * g + 128)
            k = key_value[window, 128 * g : 128 * g + 128]
            v = key_value[window, WIDTH + 128 * g : WIDTH + 128 * g + 128]
            spread_dm = spread(cot_mixed[rows, lanes])
            soft = probs[p, g]
            weighted = soft.astype(F32) * mm_t(spread_dm, v)
            total = jnp.sum(weighted, axis=-1, keepdims=True)
            cot_scores = (weighted - soft.astype(F32) * total).astype(BF)
            both = mm(cot_scores, jnp.concatenate([k, key_sides[p]], axis=1))
            cot_q.append(head_lanes(both[:, :128]))
            pairs += [both[j * QUAD : (j + 1) * QUAD, 128:] for j in range(4)]
            cot_k.append(mm_left(cot_scores, spread(query[rows, lanes])))
            cot_v.append(mm_left(soft, spread_dm))
        cot_query.append(jnp.concatenate(cot_q, axis=1))
        cot_windows.append(
            jnp.concatenate([x * SCALE for x in cot_k] + cot_v, axis=1)
        )
        pair_rows.append(jnp.concatenate(pairs, axis=1))
    from_query = mm_t((jnp.concatenate(cot_query, axis=0) * SCALE).astype(BF), w_qkv[:, :WIDTH])
    cot_normed = mm_t(jnp.concatenate(cot_windows, axis=0).astype(BF), w_qkv[:, WIDTH:])
    spread_query, spread_middle = [], []
    for p in range(4):
        for source, target in ((from_query, spread_query), (cot_middle, spread_middle)):
            part = source[p * QUAD : (p + 1) * QUAD]
            target += [part if q == 3 - p else jnp.zeros_like(part) for q in range(4)]
    cot_normed = (cot_normed + jnp.concatenate(spread_query, axis=0)) * gains[0:1]
    cot_points = normalise_back(cot_normed, unit, inv) + jnp.concatenate(spread_middle, axis=0)
    pairs = mm(cells(place, False).astype(BF), jnp.concatenate(pair_rows, axis=0).astype(BF))
    per_head = [
        [pairs[e * PITCH : e * PITCH + SPAN, 128 * h : 128 * h + 128] for e in range(3)]
        for h in range(HEADS)
    ]
    return cot_points, table_sums(per_head)


def pack_kernel(
    features, occupancy, coords, grad_out, to_y, to_x, to_xy, occupied, place, arrived
):
    pairs = [(occupancy, occupied), (coords, place)]
    for quarter, target in ((2, to_y), (1, to_x), (0, to_xy)):
        pairs.append((features, target.at[0:SLOTS]))
        rows = slice(quarter * QUAD, (quarter + 1) * QUAD)
        pairs.append((grad_out.at[rows], target.at[SLOTS : SLOTS + QUAD]))
    copies = [
        pltpu.make_async_copy(source, target, arrived.at[i])
        for i, (source, target) in enumerate(pairs)
    ]
    for copy in copies:
        copy.start()
    copies[0].wait()
    copies[1].wait()
    meta = jnp.concatenate(
        [occupied[...]] + [place[e] for e in range(3)] + [jnp.zeros((4, SLOTS), jnp.int32)], axis=0
    ).astype(F32)
    meta = jnp.concatenate([meta, jnp.zeros((8, SLOTS), F32)], axis=0)
    meta = jnp.concatenate([meta, jnp.zeros((16, SLOTS), F32)], axis=1).astype(BF)
    for target in (to_y, to_x, to_xy):
        target[SLOTS + QUAD :] = meta
    for copy in copies[2:]:
        copy.wait()


def stage_kernel(*refs):
    count = (len(refs) - 2) // 2
    sources, targets, arrived = refs[1 : 1 + count], refs[1 + count : -1], refs[-1]
    copies = [
        pltpu.make_async_copy(source, target, arrived.at[i])
        for i, (source, target) in enumerate(zip(sources, targets))
    ]
    for copy in copies:
        copy.start()
    for copy in copies:
        copy.wait()


def main_kernel(
    features, occupancy, coords, grad_out, from_y, from_x, from_xy,
    gains, tables, w_qkv, w_out, w_up, w_down,
    own_cot, own_second, back_y, back_x, back_xy, tables_out,
):
    received = (from_y, from_x, from_xy)
    points = jnp.concatenate(
        [features[...]] + [part[0:SLOTS] for part in received], axis=0
    ).astype(F32)
    grad = jnp.concatenate(
        [grad_out[3 * QUAD :]] + [part[SLOTS : SLOTS + QUAD] for part in received], axis=0
    )
    metas = [
        jnp.concatenate(
            [occupancy[...]] + [coords[e] for e in range(3)] + [jnp.zeros((4, SLOTS), jnp.int32)],
            axis=0,
        )
    ] + [
        part[SLOTS + QUAD :].astype(F32)[0:8, 0:SLOTS].astype(jnp.int32) for part in received
    ]
    quarter = iota((8, SLOTS), 1) // QUAD
    meta = jnp.zeros((8, SLOTS), jnp.int32)
    for position, part in enumerate(metas):
        moved = pltpu.roll(part, (2 * position - 3) * QUAD % SLOTS, 1)
        meta = jnp.where(quarter == position, moved, meta)
    occupied, place = meta[0:1], meta[1:4]
    half = SPAN // 2
    shifted = jnp.concatenate(
        [(place[0:1] + half) % SPAN, (place[1:2] + half) % SPAN, place[2:3]], axis=0
    )
    column = jnp.transpose(jnp.broadcast_to(occupied.astype(F32), (SLOTS, SLOTS)))
    grad = grad * jnp.concatenate([column, column], axis=1).astype(BF)
    first_weights = (w_qkv.at[0], w_out.at[0], w_up.at[0], w_down.at[0])
    second_weights = (w_qkv.at[1], w_out.at[1], w_up.at[1], w_down.at[1])
    first_out, first_saved = halo_forward(
        points, [m[1:4] for m in metas], [m[0:1] for m in metas], place, gains[0], tables[0],
        *first_weights,
    )
    hidden = first_out.astype(F32)
    second, second_saved = block_forward(
        hidden, gains[1], shifted, occupied, tables[1], *second_weights
    )
    cot, second_table = block_backward(
        grad, hidden, gains[1], shifted, second_saved, *second_weights
    )
    cot_points, first_table = halo_backward(cot, place, gains[0], first_saved, *first_weights)
    own_cot[...] = cot_points[:SLOTS]
    own_second[...] = second[:QUAD]
    for position, target in enumerate((back_y, back_x, back_xy), 1):
        target[0:SLOTS] = cot_points[position * SLOTS : (position + 1) * SLOTS].astype(BF)
        target[SLOTS:] = second[position * QUAD : (position + 1) * QUAD]
    both = first_table + pltpu.roll(second_table, 3 * PITCH, 1)
    for i in range(tables_out.shape[0]):
        tables_out[i] = both


def gather_kernel(own_cot, own_second, home_y, home_x, home_xy, occupancy, out_points, grad_points):
    total = own_cot[...]
    for part in (home_y, home_x, home_xy):
        total = total + part[0:SLOTS].astype(F32)
    grad_points[...] = total.astype(BF)
    second = jnp.concatenate([part[SLOTS:] for part in (home_xy, home_x, home_y)] + [own_second[...]], axis=0)
    column = jnp.transpose(jnp.broadcast_to(occupancy[...].astype(F32), (SLOTS, SLOTS)))
    out_points[...] = second * jnp.concatenate([column, column], axis=1).astype(BF)


def unpack_kernel(parts, out):
    total = parts[0]
    for i in range(1, parts.shape[0]):
        total = total + parts[i]
    for k in range(2):
        for e in range(3):
            start = (3 * k + e) * PITCH
            moved = total if start == 0 else pltpu.roll(total, 128 - start, 1)
            out[k, e] = moved[:, : out.shape[-1]]


def call(kernel, shapes, *args, far=None, scratch=()):
    options = {}
    if far is not None:
        args = args[:far] + tuple(in_hbm(a) for a in args[far:])
        options["in_specs"] = [pl.BlockSpec(memory_space=pl.ANY)] * far + [
            pl.BlockSpec(memory_space=pltpu.HBM)
        ] * (len(args) - far)
    return pl.pallas_call(
        kernel,
        out_shape=[jax.ShapeDtypeStruct(s, d) for s, d in shapes],
        scratch_shapes=scratch,
        compiler_params=pltpu.CompilerParams(vmem_limit_bytes=VMEM_LIMIT),
        interpret=INTERPRET,
        **options,
    )(*args)


def in_hbm(value):
    return value if INTERPRET else pltpu.with_memory_space_constraint(value, pltpu.HBM)


def on_device(
    gx, gy, phases,
    features, occupancy, coords, norm_gains, bias_tables, w_qkv, w_out, w_up, w_down, grad_out,
):
    size_x = lax.axis_size(gx)
    size_y = lax.axis_size(gy)

    def move(value, step_x, step_y):
        pairs = []
        for i in range(size_x):
            for j in range(size_y):
                target = (i + step_x) % size_x * size_y + (j + step_y) % size_y
                pairs.append((i * size_y + j, target))
        return lax.ppermute(value, gx + gy, pairs)

    points, occupied, grad = features[0, 0], occupancy[0], grad_out[0, 0]
    place = jnp.swapaxes(coords[0], 0, 1)
    packet, reply = ((SLOTS + QUAD + 16, WIDTH), BF), ((SLOTS + QUAD, WIDTH), BF)
    to_y, to_x, to_xy = call(
        pack_kernel, [packet] * 3, points, occupied, place, grad, far=0,
        scratch=[pltpu.VMEM(occupied.shape, jnp.int32), pltpu.VMEM(place.shape, jnp.int32), pltpu.SemaphoreType.DMA((8,))],
    )
    sources = (points, occupied, place, grad, norm_gains, bias_tables, w_qkv, w_out, w_up, w_down)
    staged = call(
        stage_kernel, [(a.shape, a.dtype) for a in sources], to_y, *sources, far=1,
        scratch=[pltpu.SemaphoreType.DMA((len(sources),))],
    )
    first = lax.axis_size(phases[0])
    own_cot, own_second, back_y, back_x, back_xy, tables = call(
        main_kernel,
        [((SLOTS, WIDTH), F32), ((QUAD, WIDTH), BF)] + [reply] * 3 + [((first, HEADS, 128), F32)],
        *staged[:4], move(to_y, 0, -1), move(to_x, -1, 0), move(to_xy, -1, -1), *staged[4:],
    )
    home = move(back_y, 0, 1), move(back_x, 1, 0), move(back_xy, 1, 1)
    for phase, after in zip(phases, phases[1:] + (None,)):
        tables = lax.all_to_all(tables, phase, 0, 0)
        if after is not None:
            tables = jnp.broadcast_to(
                jnp.sum(tables, axis=0)[None], (lax.axis_size(after), HEADS, 128)
            )
    (grad_tables,) = call(unpack_kernel, [(bias_tables.shape, F32)], tables)
    out_points, grad_points = call(
        gather_kernel, [((SLOTS, WIDTH), BF)] * 2, own_cot, own_second, *home, staged[1]
    )
    return out_points[None, None], grad_points[None, None], grad_tables


def solution(mesh):
    shape = tuple(mesh.shape[a] for a in ("gx", "gy"))
    if shape == (16, 32):
        fine = Mesh(mesh.devices.reshape(2, 4, 2, 8, 4), ("zh", "y", "c", "zl", "x"))
        gx, gy = ("zh", "y", "c"), ("zl", "x")
        phases = (("y", "c", "x"), ("zh", "zl"))
    else:
        fine = Mesh(mesh.devices, ("gx", "gy"))
        gx, gy, phases = ("gx",), ("gy",), (("gx",), ("gy",))
    grid = P(gx, gy, None, None)
    return jax.shard_map(
        partial(on_device, gx, gy, phases),
        mesh=fine,
        in_specs=(grid, P(gx, gy, None), grid, P(), P(), P(), P(), P(), P(), grid),
        out_specs=(grid, grid, P()),
        check_vma=False,
    )
```

```python
from functools import partial

import jax
import jax.numpy as jnp
from jax import lax
from jax.experimental import pallas as pl
from jax.experimental.pallas import tpu as pltpu
from jax.sharding import Mesh
from jax.sharding import PartitionSpec as P

INTERPRET = False
EPS = 1e-05
BF = jnp.bfloat16
F32 = jnp.float32
SLOTS, WIDTH, HEADS, HD, QUAD = 128, 256, 8, 32, 32
SPAN, PITCH = 8, 16
SCALE = HD ** (-0.5)
MASKED = -1e30
VMEM_LIMIT = 24 * 1024 * 1024


def mm(a, b):
    return lax.dot_general(a, b, (((1,), (0,)), ((), ())), preferred_element_type=F32)


def mm_t(a, b):
    return lax.dot_general(a, b, (((1,), (1,)), ((), ())), preferred_element_type=F32)


def iota(shape, axis):
    return lax.broadcasted_iota(jnp.int32, shape, axis)


def normalise(values):
    centred = values - jnp.mean(values, axis=-1, keepdims=True)
    inv = lax.rsqrt(jnp.mean(centred * centred, axis=-1, keepdims=True) + EPS)
    return centred * inv, inv


def normalise_back(cot, unit, inv):
    return inv * (
        cot
        - jnp.mean(cot, axis=-1, keepdims=True)
        - unit * jnp.mean(cot * unit, axis=-1, keepdims=True)
    )


def cells(coords, mirrored):
    row = iota((PITCH, SLOTS), 0)
    if mirrored:
        row = SPAN - 1 - row
    return jnp.concatenate(
        [(coords[e : e + 1] == row).astype(F32) for e in range(3)], axis=0
    )


def query_cells(coords):
    ones = jnp.where(iota((PITCH, SLOTS), 0) == 0, 1.0, 0.0)
    return jnp.concatenate(
        [cells(coords, True), ones, jnp.zeros((SLOTS - 4 * PITCH, SLOTS), F32)], axis=0
    )


def key_cells(coords, occupied):
    mirrored = cells(coords, True)
    mask = jnp.where((iota((PITCH, SLOTS), 0) == 0) & (occupied <= 0), MASKED, 0.0)
    return jnp.concatenate([mirrored, mirrored, mask, jnp.zeros((PITCH, SLOTS), F32)], axis=0)


def table_matrix(table):
    lane = iota((SPAN, 128), 1)
    wide = []
    for e in range(3):
        row = jnp.concatenate(
            [table[e] * (1.0 / SCALE), jnp.zeros((HEADS, 128 - table.shape[-1]), F32)], axis=1
        )
        start = e * PITCH - (SPAN - 1)
        wide.append(
            pltpu.roll(row, start % 128, 1) + pltpu.roll(row, (start + 3 * PITCH) % 128, 1)
        )
    columns = []
    for h in range(HEADS):
        rows = []
        for e in range(3):
            value = pltpu.roll(
                jnp.broadcast_to(wide[e][h : h + 1], (SPAN, 128)), 0, 1, stride=1, stride_axis=0
            )
            high = value.astype(BF).astype(F32)
            value = jnp.where(lane < 3 * PITCH, high, value - high)
            base = lane % (3 * PITCH) - e * PITCH
            keep = (base >= 0) & (base < SPAN) & (lane < 6 * PITCH)
            rows += [jnp.where(keep, value, 0.0), jnp.zeros((SPAN, 128), F32)]
        one = (iota((PITCH, 128), 0) == 0) & (iota((PITCH, 128), 1) == 6 * PITCH)
        rows += [jnp.where(one, 1.0, 0.0), jnp.zeros((128 - 4 * PITCH, 128), F32)]
        columns.append(jnp.concatenate(rows, axis=0))
    return jnp.concatenate(columns, axis=1).astype(BF)


def spread(group):
    head = iota(group.shape, 1) // HD
    return jnp.concatenate(
        [jnp.where(head == j, group, jnp.zeros_like(group)) for j in range(4)], axis=0
    )


def side_by_side(stack):
    return jnp.concatenate([stack[j * SLOTS : (j + 1) * SLOTS] for j in range(4)], axis=1)


def softmax(scores):
    weights = jnp.exp((scores - jnp.max(scores, axis=-1, keepdims=True)) * SCALE)
    return (weights * (1.0 / jnp.sum(weights, axis=-1, keepdims=True))).astype(BF)


def gelu_parts(v):
    c = 0.7978845608028654
    t = jnp.tanh(c * (v + 0.044715 * (v * v * v)))
    return 0.5 * v * (1.0 + t), t


def gelu_slope(v):
    c = 0.7978845608028654
    t = jnp.tanh(c * (v + 0.044715 * (v * v * v)))
    return 0.5 * (1.0 + t) + 0.5 * v * (1.0 - t * t) * c * (1.0 + 3 * 0.044715 * (v * v))


def block_forward(hidden, gains, coords, occupied, table, w_qkv, w_out, w_up, w_down):
    unit, _ = normalise(hidden)
    projected = mm((unit * gains[0:1]).astype(BF), w_qkv[...]).astype(BF)
    query_side = jnp.transpose(query_cells(coords)).astype(BF)
    key_side = jnp.transpose(key_cells(coords, occupied)).astype(BF)
    bias_left = mm(query_side, table_matrix(table)).astype(BF)
    probs, mixed = [], []
    for g in range(2):
        q = projected[:, 128 * g : 128 * g + 128]
        k = projected[:, 256 + 128 * g : 256 + 128 * g + 128]
        v = projected[:, 512 + 128 * g : 512 + 128 * g + 128]
        lefts = jnp.concatenate(
            [bias_left[:, 128 * h : 128 * h + 128] for h in range(4 * g, 4 * g + 4)], axis=0
        )
        scores = mm_t(
            jnp.concatenate([spread(q), lefts], axis=1), jnp.concatenate([k, key_side], axis=1)
        )
        soft = softmax(scores)
        probs.append(soft)
        mixed.append(mm(side_by_side(soft), spread(v)))
    middle = hidden + mm(jnp.concatenate(mixed, axis=1).astype(BF), w_out[...])
    unit_two, _ = normalise(middle)
    up = mm((unit_two * gains[1:2]).astype(BF), w_up[...])
    expanded, _ = gelu_parts(up)
    out = middle + mm(expanded.astype(BF), w_down[...])
    return out.astype(BF), (projected, probs, middle, up)


def feed_forward_back(cot, gains, middle, up, w_out, w_up, w_down):
    unit, inv = normalise(middle)
    cot_up = mm_t(cot, w_down[...]) * gelu_slope(up)
    cot_two = mm_t(cot_up.astype(BF), w_up[...]) * gains[1:2]
    cot_middle = cot.astype(F32) + normalise_back(cot_two, unit, inv)
    return cot_middle, mm_t(cot_middle.astype(BF), w_out[...]).astype(BF)


def table_sums(per_head):
    lane = iota((SPAN, 128), 1)
    tables = []
    for blocks in per_head:
        value = jnp.where(lane < PITCH, blocks[0], jnp.where(lane < 2 * PITCH, blocks[1], blocks[2]))
        value = jnp.where(lane < 3 * PITCH, value, 0.0)
        value = pltpu.roll(value, 0, 1, stride=1, stride_axis=0)
        tables.append(jnp.sum(value, axis=0, keepdims=True))
    return jnp.concatenate(tables, axis=0)


def block_backward(cot, hidden, gains, coords, saved, w_qkv, w_out, w_up, w_down, with_table=True):
    projected, probs, middle, up = saved
    cot_middle, cot_mixed = feed_forward_back(cot, gains, middle, up, w_out, w_up, w_down)
    cells_t = cells(coords, False).astype(BF)
    blank = jnp.zeros((SLOTS - 3 * PITCH, SLOTS), F32)
    cells_key = jnp.transpose(jnp.concatenate([cells(coords, True), blank], axis=0)).astype(BF)
    cot_q, cot_k, cot_v, pair_sums = [], [], [], []
    for g in range(2):
        q = projected[:, 128 * g : 128 * g + 128]
        k = projected[:, 256 + 128 * g : 256 + 128 * g + 128]
        v = projected[:, 512 + 128 * g : 512 + 128 * g + 128]
        dm = cot_mixed[:, 128 * g : 128 * g + 128]
        q_t = jnp.transpose(q.astype(F32)).astype(BF)
        dm_t = jnp.transpose(dm.astype(F32)).astype(BF)
        soft = probs[g]
        cot_soft = mm_t(spread(dm), v)
        weighted = soft.astype(F32) * cot_soft
        total = jnp.sum(weighted, axis=-1, keepdims=True)
        cot_scores = (weighted - soft.astype(F32) * total).astype(BF)
        cot_q.append(mm(side_by_side(cot_scores), spread(k)) * SCALE)
        k_rows, v_rows = [], []
        for j in range(4):
            rows = slice(j * SLOTS, (j + 1) * SLOTS)
            lanes = slice(j * HD, (j + 1) * HD)
            left = jnp.concatenate([q_t[lanes], cells_t], axis=0) if with_table else q_t[lanes]
            both = mm(left, cot_scores[rows])
            k_rows.append(both[:HD])
            pair_sums.append(both[HD:])
            v_rows.append(mm(dm_t[lanes], soft[rows]))
        cot_k.append(jnp.transpose(jnp.concatenate(k_rows, axis=0)) * SCALE)
        cot_v.append(jnp.transpose(jnp.concatenate(v_rows, axis=0)))
    cot_projected = jnp.concatenate(cot_q + cot_k + cot_v, axis=1).astype(BF)
    cot_normed = mm_t(cot_projected, w_qkv[...]) * gains[0:1]
    unit, inv = normalise(hidden)
    cot_hidden = cot_middle + normalise_back(cot_normed, unit, inv)
    if not with_table:
        return cot_hidden.astype(BF), None
    pairs = mm(jnp.concatenate(pair_sums, axis=0).astype(BF), cells_key)
    per_head = [
        [pairs[(3 * h + e) * PITCH : (3 * h + e) * PITCH + SPAN] for e in range(3)]
        for h in range(HEADS)
    ]
    return cot_hidden.astype(BF), table_sums(per_head)


def head_lanes(stack):
    rows = stack.shape[0] // 4
    head = iota((rows, 128), 1) // HD
    out = jnp.zeros((rows, 128), stack.dtype)
    for j in range(4):
        out = jnp.where(head == j, stack[j * rows : (j + 1) * rows], out)
    return out


def halo_forward(points, places, occupieds, place, gains, table, w_qkv, w_out, w_up, w_down):
    unit, _ = normalise(points)
    normed = (unit * gains[0:1]).astype(BF)
    key_value = mm(normed, w_qkv[:, WIDTH:]).astype(BF)
    quarters = [slice(p * SLOTS + (3 - p) * QUAD, p * SLOTS + (4 - p) * QUAD) for p in range(4)]
    query = mm(jnp.concatenate([normed[r] for r in quarters], axis=0), w_qkv[:, :WIDTH]).astype(BF)
    hidden = jnp.concatenate([points[r] for r in quarters], axis=0)
    query_side = jnp.transpose(query_cells(place)).astype(BF)
    bias_left = mm(query_side, table_matrix(table)).astype(BF)
    probs, mixed, key_sides = {}, [], []
    for p in range(4):
        key_side = jnp.transpose(key_cells(places[p], occupieds[p])).astype(BF)
        key_sides.append(key_side)
        rows, window = slice(p * QUAD, (p + 1) * QUAD), slice(p * SLOTS, (p + 1) * SLOTS)
        groups = []
        for g in range(2):
            lanes = slice(128 * g, 128 * g + 128)
            k = key_value[window, 128 * g : 128 * g + 128]
            v = key_value[window, WIDTH + 128 * g : WIDTH + 128 * g + 128]
            lefts = jnp.concatenate(
                [bias_left[rows, 128 * h : 128 * h + 128] for h in range(4 * g, 4 * g + 4)], axis=0
            )
            scores = mm_t(
                jnp.concatenate([spread(query[rows, lanes]), lefts], axis=1),
                jnp.concatenate([k, key_side], axis=1),
            )
            probs[p, g] = softmax(scores)
            groups.append(head_lanes(mm(probs[p, g], v)))
        mixed.append(jnp.concatenate(groups, axis=1))
    middle = hidden + mm(jnp.concatenate(mixed, axis=0).astype(BF), w_out[...])
    unit_two, _ = normalise(middle)
    up = mm((unit_two * gains[1:2]).astype(BF), w_up[...])
    expanded, _ = gelu_parts(up)
    out = middle + mm(expanded.astype(BF), w_down[...])
    return out.astype(BF), (key_value, probs, key_sides, middle, up)


def halo_table(cot, place, gains, saved, w_out, w_up, w_down):
    key_value, probs, key_sides, middle, up = saved
    _, cot_mixed = feed_forward_back(cot, gains, middle, up, w_out, w_up, w_down)
    pair_rows = []
    for p in range(4):
        rows, window = slice(p * QUAD, (p + 1) * QUAD), slice(p * SLOTS, (p + 1) * SLOTS)
        pairs = []
        for g in range(2):
            v = key_value[window, WIDTH + 128 * g : WIDTH + 128 * g + 128]
            soft = probs[p, g].astype(F32)
            weighted = soft * mm_t(spread(cot_mixed[rows, 128 * g : 128 * g + 128]), v)
            total = jnp.sum(weighted, axis=-1, keepdims=True)
            both = mm((weighted - soft * total).astype(BF), key_sides[p])
            pairs += [both[j * QUAD : (j + 1) * QUAD] for j in range(4)]
        pair_rows.append(jnp.concatenate(pairs, axis=1))
    pairs = mm(cells(place, False).astype(BF), jnp.concatenate(pair_rows, axis=0).astype(BF))
    return table_sums(
        [
            [pairs[e * PITCH : e * PITCH + SPAN, 128 * h : 128 * h + 128] for e in range(3)]
            for h in range(HEADS)
        ]
    )


def pack_kernel(
    features, occupancy, coords, grad_out, to_y, to_x, to_xy, occupied, place, arrived
):
    pairs = [(occupancy, occupied), (coords, place)]
    for quarter, target in ((2, to_y), (1, to_x), (0, to_xy)):
        pairs.append((features, target.at[0:SLOTS]))
        rows = slice(quarter * QUAD, (quarter + 1) * QUAD)
        pairs.append((grad_out.at[rows], target.at[SLOTS : SLOTS + QUAD]))
    copies = [
        pltpu.make_async_copy(source, target, arrived.at[i])
        for i, (source, target) in enumerate(pairs)
    ]
    for copy in copies:
        copy.start()
    copies[0].wait()
    copies[1].wait()
    meta = jnp.concatenate(
        [occupied[...]] + [place[e] for e in range(3)] + [jnp.zeros((4, SLOTS), jnp.int32)], axis=0
    ).astype(F32)
    meta = jnp.concatenate([meta, jnp.zeros((8, SLOTS), F32)], axis=0)
    meta = jnp.concatenate([meta, jnp.zeros((16, SLOTS), F32)], axis=1).astype(BF)
    for target in (to_y, to_x, to_xy):
        target[SLOTS + QUAD :] = meta
    for copy in copies[2:]:
        copy.wait()


def stage_kernel(*refs):
    count = (len(refs) - 2) // 2
    sources, targets, arrived = refs[1 : 1 + count], refs[1 + count : -1], refs[-1]
    copies = [
        pltpu.make_async_copy(source, target, arrived.at[i])
        for i, (source, target) in enumerate(zip(sources, targets))
    ]
    for copy in copies:
        copy.start()
    for copy in copies:
        copy.wait()


def main_kernel(
    features, occupancy, coords, grad_out, from_y, from_x, from_xy,
    gains, tables, w_qkv, w_out, w_up, w_down,
    own, back_y, back_x, back_xy, tables_out,
):
    received = (from_y, from_x, from_xy)
    points = jnp.concatenate(
        [features[...]] + [part[0:SLOTS] for part in received], axis=0
    ).astype(F32)
    grad = jnp.concatenate(
        [grad_out[3 * QUAD :]] + [part[SLOTS : SLOTS + QUAD] for part in received], axis=0
    )
    metas = [
        jnp.concatenate(
            [occupancy[...]] + [coords[e] for e in range(3)] + [jnp.zeros((4, SLOTS), jnp.int32)],
            axis=0,
        )
    ] + [
        part[SLOTS + QUAD :].astype(F32)[0:8, 0:SLOTS].astype(jnp.int32) for part in received
    ]
    quarter = iota((8, SLOTS), 1) // QUAD
    meta = jnp.zeros((8, SLOTS), jnp.int32)
    for position, part in enumerate(metas):
        moved = pltpu.roll(part, (2 * position - 3) * QUAD % SLOTS, 1)
        meta = jnp.where(quarter == position, moved, meta)
    occupied, place = meta[0:1], meta[1:4]
    half = SPAN // 2
    shifted = jnp.concatenate(
        [(place[0:1] + half) % SPAN, (place[1:2] + half) % SPAN, place[2:3]], axis=0
    )
    column = jnp.transpose(jnp.broadcast_to(occupied.astype(F32), (SLOTS, SLOTS)))
    grad = grad * jnp.concatenate([column, column], axis=1).astype(BF)
    first_weights = (w_qkv.at[0], w_out.at[0], w_up.at[0], w_down.at[0])
    second_weights = (w_qkv.at[1], w_out.at[1], w_up.at[1], w_down.at[1])
    first_out, first_saved = halo_forward(
        points, [m[1:4] for m in metas], [m[0:1] for m in metas], place, gains[0], tables[0],
        *first_weights,
    )
    hidden = first_out.astype(F32)
    second, second_saved = block_forward(
        hidden, gains[1], shifted, occupied, tables[1], *second_weights
    )
    cot, second_table = block_backward(
        grad, hidden, gains[1], shifted, second_saved, *second_weights
    )
    first_table = halo_table(cot, place, gains[0], first_saved, *first_weights[1:])
    for position, target in enumerate((own, back_y, back_x, back_xy)):
        rows = slice(position * QUAD, (position + 1) * QUAD)
        target[0:QUAD] = second[rows]
        target[QUAD:] = cot[rows]
    both = first_table + pltpu.roll(second_table, 3 * PITCH, 1)
    for i in range(tables_out.shape[0]):
        tables_out[i] = both.astype(BF)


def window_kernel(
    home_xy, home_x, home_y, own, features, occupancy, coords,
    gains, tables, w_qkv, w_out, w_up, w_down, out_points, grad_points,
):
    parts = (home_xy, home_x, home_y, own)
    second = jnp.concatenate([part[0:QUAD] for part in parts], axis=0)
    cot = jnp.concatenate([part[QUAD:] for part in parts], axis=0)
    column = jnp.transpose(jnp.broadcast_to(occupancy[...].astype(F32), (SLOTS, SLOTS)))
    out_points[...] = second * jnp.concatenate([column, column], axis=1).astype(BF)
    place = jnp.concatenate([coords[e] for e in range(3)], axis=0)
    weights = (w_qkv.at[0], w_out.at[0], w_up.at[0], w_down.at[0])
    points = features[...].astype(F32)
    _, saved = block_forward(points, gains[0], place, occupancy[...], tables[0], *weights)
    grad_points[...], _ = block_backward(
        cot, points, gains[0], place, saved, *weights, with_table=False
    )


def unpack_kernel(parts, out):
    total = parts[0].astype(F32)
    for i in range(1, parts.shape[0]):
        total = total + parts[i].astype(F32)
    for k in range(2):
        for e in range(3):
            start = (3 * k + e) * PITCH
            moved = total if start == 0 else pltpu.roll(total, 128 - start, 1)
            out[k, e] = moved[:, : out.shape[-1]]


def call(kernel, shapes, *args, far=None, scratch=()):
    options = {}
    if far is not None:
        args = args[:far] + tuple(in_hbm(a) for a in args[far:])
        options["in_specs"] = [pl.BlockSpec(memory_space=pl.ANY)] * far + [
            pl.BlockSpec(memory_space=pltpu.HBM)
        ] * (len(args) - far)
    return pl.pallas_call(
        kernel,
        out_shape=[jax.ShapeDtypeStruct(s, d) for s, d in shapes],
        scratch_shapes=scratch,
        compiler_params=pltpu.CompilerParams(vmem_limit_bytes=VMEM_LIMIT),
        interpret=INTERPRET,
        **options,
    )(*args)


def in_hbm(value):
    return value if INTERPRET else pltpu.with_memory_space_constraint(value, pltpu.HBM)


def on_device(
    gx, gy, phases,
    features, occupancy, coords, norm_gains, bias_tables, w_qkv, w_out, w_up, w_down, grad_out,
):
    size_x = lax.axis_size(gx)
    size_y = lax.axis_size(gy)

    def move(value, step_x, step_y):
        pairs = []
        for i in range(size_x):
            for j in range(size_y):
                target = (i + step_x) % size_x * size_y + (j + step_y) % size_y
                pairs.append((i * size_y + j, target))
        return lax.ppermute(value, gx + gy, pairs)

    points, occupied, grad = features[0, 0], occupancy[0], grad_out[0, 0]
    place = jnp.swapaxes(coords[0], 0, 1)
    packet, reply = ((SLOTS + QUAD + 16, WIDTH), BF), ((2 * QUAD, WIDTH), BF)
    to_y, to_x, to_xy = call(
        pack_kernel, [packet] * 3, points, occupied, place, grad, far=0,
        scratch=[pltpu.VMEM(occupied.shape, jnp.int32), pltpu.VMEM(place.shape, jnp.int32), pltpu.SemaphoreType.DMA((8,))],
    )
    sources = (points, occupied, place, grad, norm_gains, bias_tables, w_qkv, w_out, w_up, w_down)
    staged = call(
        stage_kernel, [(a.shape, a.dtype) for a in sources], to_y, *sources, far=1,
        scratch=[pltpu.SemaphoreType.DMA((len(sources),))],
    )
    first = lax.axis_size(phases[0])
    own, back_y, back_x, back_xy, tables = call(
        main_kernel,
        [reply] * 4 + [((first, HEADS, 128), BF)],
        *staged[:4], move(to_y, 0, -1), move(to_x, -1, 0), move(to_xy, -1, -1), *staged[4:],
    )
    home_y = move(back_y, 0, 1)
    home_x = move(back_x, 1, 0)
    home_xy = move(back_xy, 1, 1)
    tables = lax.all_to_all(tables, phases[0], 0, 0)
    total = jnp.sum(tables.astype(F32), axis=0).astype(BF)
    tables = jnp.broadcast_to(total[None], (lax.axis_size(phases[1]), HEADS, 128))
    tables = lax.all_to_all(tables, phases[1], 0, 0)
    (grad_tables,) = call(unpack_kernel, [(bias_tables.shape, F32)], tables)
    out_points, grad_points = call(
        window_kernel, [((SLOTS, WIDTH), BF)] * 2, home_xy, home_x, home_y, own, *staged[:3], *staged[4:]
    )
    return out_points[None, None], grad_points[None, None], grad_tables


def solution(mesh):
    shape = tuple(mesh.shape[a] for a in ("gx", "gy"))
    if shape == (16, 32):
        fine = Mesh(mesh.devices.reshape(2, 4, 2, 8, 4), ("zh", "y", "c", "zl", "x"))
        gx, gy = ("zh", "y", "c"), ("zl", "x")
        phases = (("y", "c", "x"), ("zh", "zl"))
    else:
        fine = Mesh(mesh.devices, ("gx", "gy"))
        gx, gy, phases = ("gx",), ("gy",), (("gx",), ("gy",))
    grid = P(gx, gy, None, None)
    return jax.shard_map(
        partial(on_device, gx, gy, phases),
        mesh=fine,
        in_specs=(grid, P(gx, gy, None), grid, P(), P(), P(), P(), P(), P(), grid),
        out_specs=(grid, grid, P()),
        check_vma=False,
    )
```

```python
from functools import partial

import jax
import jax.numpy as jnp
from jax import lax
from jax.experimental import pallas as pl
from jax.experimental.pallas import tpu as pltpu
from jax.sharding import Mesh
from jax.sharding import PartitionSpec as P

INTERPRET = False
EPS = 1e-05
BF = jnp.bfloat16
F32 = jnp.float32
SLOTS, WIDTH, HEADS, HD, QUAD = 128, 256, 8, 32, 32
SPAN, PITCH = 8, 16
SCALE = HD ** (-0.5)
MASKED = -1e30
COST = 10_000_000_000
VMEM_LIMIT = 24 * 1024 * 1024


def mm(a, b):
    return lax.dot_general(a, b, (((1,), (0,)), ((), ())), preferred_element_type=F32)


def mm_t(a, b):
    return lax.dot_general(a, b, (((1,), (1,)), ((), ())), preferred_element_type=F32)


def iota(shape, axis):
    return lax.broadcasted_iota(jnp.int32, shape, axis)


def normalise(values):
    centred = values - jnp.mean(values, axis=-1, keepdims=True)
    inv = lax.rsqrt(jnp.mean(centred * centred, axis=-1, keepdims=True) + EPS)
    return centred * inv, inv


def normalise_back(cot, unit, inv):
    return inv * (
        cot
        - jnp.mean(cot, axis=-1, keepdims=True)
        - unit * jnp.mean(cot * unit, axis=-1, keepdims=True)
    )


def cells(coords, mirrored):
    row = iota((PITCH, SLOTS), 0)
    if mirrored:
        row = SPAN - 1 - row
    return jnp.concatenate(
        [(coords[e : e + 1] == row).astype(F32) for e in range(3)], axis=0
    )


def query_cells(coords):
    ones = jnp.where(iota((PITCH, SLOTS), 0) == 0, 1.0, 0.0)
    return jnp.concatenate(
        [cells(coords, True), ones, jnp.zeros((SLOTS - 4 * PITCH, SLOTS), F32)], axis=0
    )


def key_cells(coords, occupied):
    mirrored = cells(coords, True)
    mask = jnp.where((iota((PITCH, SLOTS), 0) == 0) & (occupied <= 0), MASKED, 0.0)
    return jnp.concatenate([mirrored, mirrored, mask, jnp.zeros((PITCH, SLOTS), F32)], axis=0)


def table_matrix(table):
    lane = iota((SPAN, 128), 1)
    wide = []
    for e in range(3):
        row = jnp.concatenate(
            [table[e] * (1.0 / SCALE), jnp.zeros((HEADS, 128 - table.shape[-1]), F32)], axis=1
        )
        start = e * PITCH - (SPAN - 1)
        wide.append(
            pltpu.roll(row, start % 128, 1) + pltpu.roll(row, (start + 3 * PITCH) % 128, 1)
        )
    columns = []
    for h in range(HEADS):
        rows = []
        for e in range(3):
            value = pltpu.roll(
                jnp.broadcast_to(wide[e][h : h + 1], (SPAN, 128)), 0, 1, stride=1, stride_axis=0
            )
            high = value.astype(BF).astype(F32)
            value = jnp.where(lane < 3 * PITCH, high, value - high)
            base = lane % (3 * PITCH) - e * PITCH
            keep = (base >= 0) & (base < SPAN) & (lane < 6 * PITCH)
            rows += [jnp.where(keep, value, 0.0), jnp.zeros((SPAN, 128), F32)]
        one = (iota((PITCH, 128), 0) == 0) & (iota((PITCH, 128), 1) == 6 * PITCH)
        rows += [jnp.where(one, 1.0, 0.0), jnp.zeros((128 - 4 * PITCH, 128), F32)]
        columns.append(jnp.concatenate(rows, axis=0))
    return jnp.concatenate(columns, axis=1).astype(BF)


def spread(group):
    head = iota(group.shape, 1) // HD
    return jnp.concatenate(
        [jnp.where(head == j, group, jnp.zeros_like(group)) for j in range(4)], axis=0
    )


def side_by_side(stack):
    return jnp.concatenate([stack[j * SLOTS : (j + 1) * SLOTS] for j in range(4)], axis=1)


def attend(scores, values):
    tops = [jnp.max(x, axis=-1, keepdims=True) for x in scores]
    factor = SCALE * 1.4426950408889634
    weights = [jnp.exp2((x - top) * factor) for x, top in zip(scores, tops)]
    ones = jnp.ones_like(values[0])
    both = [mm(w.astype(BF), jnp.concatenate([v, ones], axis=1)) for w, v in zip(weights, values)]
    shares = [1.0 / x[:, 128:] for x in both]
    return (
        [w * share for w, share in zip(weights, shares)],
        [head_lanes(x[:, :128] * share) for x, share in zip(both, shares)],
    )


def attend_back(soft, mixed, cot_mixed, v):
    product = mixed * cot_mixed.astype(F32)
    high = product.astype(BF)
    low = (product - high.astype(F32)).astype(BF)
    ones = jnp.ones_like(v)
    left = jnp.concatenate([spread(cot_mixed), spread(-high), spread(-low)], axis=1)
    return (soft * mm_t(left, jnp.concatenate([v, ones, ones], axis=1))).astype(BF)


def gelu_and_slope(v):
    c = 0.7978845608028654
    square = v * v
    t = jnp.tanh(v * (c + (c * 0.044715) * square))
    half = 0.5 + 0.5 * t
    return v * half, half + (0.5 * v) * (1.0 - t * t) * (c + (3 * c * 0.044715) * square)


def block_forward(hidden, gains, coords, occupied, table, w_qkv, w_out, w_up, w_down):
    unit, inv = normalise(hidden)
    projected = mm((unit * gains[0:1]).astype(BF), w_qkv[...]).astype(BF)
    query_side = jnp.transpose(query_cells(coords)).astype(BF)
    key_side = jnp.transpose(key_cells(coords, occupied)).astype(BF)
    bias_left = mm(query_side, table_matrix(table)).astype(BF)
    scores, values = [], []
    for g in range(2):
        q = projected[:, 128 * g : 128 * g + 128]
        k = projected[:, 256 + 128 * g : 256 + 128 * g + 128]
        values.append(projected[:, 512 + 128 * g : 512 + 128 * g + 128])
        lefts = jnp.concatenate(
            [bias_left[:, 128 * h : 128 * h + 128] for h in range(4 * g, 4 * g + 4)], axis=0
        )
        scores.append(
            mm_t(jnp.concatenate([spread(q), lefts], axis=1), jnp.concatenate([k, key_side], axis=1))
        )
    probs, mixed = attend(scores, values)
    mixed = jnp.concatenate(mixed, axis=1)
    middle = hidden + mm(mixed.astype(BF), w_out[...])
    unit_two, inv_two = normalise(middle)
    up = mm((unit_two * gains[1:2]).astype(BF), w_up[...])
    expanded, slope = gelu_and_slope(up)
    out = middle + mm(expanded.astype(BF), w_down[...])
    return out.astype(BF), (projected, probs, mixed, unit, inv, unit_two, inv_two, slope)


def feed_forward_back(cot, gains, unit, inv, slope, w_out, w_up, w_down):
    cot_up = mm_t(cot, w_down[...]) * slope
    cot_two = mm_t(cot_up.astype(BF), w_up[...]) * gains[1:2]
    cot_middle = cot.astype(F32) + normalise_back(cot_two, unit, inv)
    return cot_middle, mm_t(cot_middle.astype(BF), w_out[...]).astype(BF)


def table_sums(per_head):
    lane = iota((SPAN, 128), 1)
    tables = []
    for blocks in per_head:
        value = jnp.where(lane < PITCH, blocks[0], jnp.where(lane < 2 * PITCH, blocks[1], blocks[2]))
        value = jnp.where(lane < 3 * PITCH, value, 0.0)
        value = pltpu.roll(value, 0, 1, stride=1, stride_axis=0)
        tables.append(jnp.sum(value, axis=0, keepdims=True))
    return jnp.concatenate(tables, axis=0)


def block_backward(cot, gains, coords, saved, w_qkv, w_out, w_up, w_down, with_table=True):
    projected, probs, mixed, unit, inv, unit_two, inv_two, slope = saved
    cot_middle, cot_mixed = feed_forward_back(
        cot, gains, unit_two, inv_two, slope, w_out, w_up, w_down
    )
    cells_t = cells(coords, False).astype(BF)
    blank = jnp.zeros((SLOTS - 3 * PITCH, SLOTS), F32)
    cells_key = jnp.transpose(jnp.concatenate([cells(coords, True), blank], axis=0)).astype(BF)
    cot_q, cot_k, cot_v, pair_sums = [], [], [], []
    for g in range(2):
        q = projected[:, 128 * g : 128 * g + 128]
        k = projected[:, 256 + 128 * g : 256 + 128 * g + 128]
        v = projected[:, 512 + 128 * g : 512 + 128 * g + 128]
        dm = cot_mixed[:, 128 * g : 128 * g + 128]
        q_t = jnp.transpose(q.astype(F32)).astype(BF)
        dm_t = jnp.transpose(dm.astype(F32)).astype(BF)
        cot_scores = attend_back(probs[g], mixed[:, 128 * g : 128 * g + 128], dm, v)
        soft = probs[g].astype(BF)
        cot_q.append(mm(side_by_side(cot_scores), spread(k)) * SCALE)
        k_rows, v_rows = [], []
        for j in range(4):
            rows = slice(j * SLOTS, (j + 1) * SLOTS)
            lanes = slice(j * HD, (j + 1) * HD)
            left = jnp.concatenate([q_t[lanes], cells_t], axis=0) if with_table else q_t[lanes]
            both = mm(left, cot_scores[rows])
            k_rows.append(both[:HD])
            pair_sums.append(both[HD:])
            v_rows.append(mm(dm_t[lanes], soft[rows]))
        cot_k.append(jnp.transpose(jnp.concatenate(k_rows, axis=0)) * SCALE)
        cot_v.append(jnp.transpose(jnp.concatenate(v_rows, axis=0)))
    cot_projected = jnp.concatenate(cot_q + cot_k + cot_v, axis=1).astype(BF)
    cot_normed = mm_t(cot_projected, w_qkv[...]) * gains[0:1]
    cot_hidden = cot_middle + normalise_back(cot_normed, unit, inv)
    if not with_table:
        return cot_hidden.astype(BF), None
    pairs = mm(jnp.concatenate(pair_sums, axis=0).astype(BF), cells_key)
    per_head = [
        [pairs[(3 * h + e) * PITCH : (3 * h + e) * PITCH + SPAN] for e in range(3)]
        for h in range(HEADS)
    ]
    return cot_hidden.astype(BF), table_sums(per_head)


def head_lanes(stack):
    rows = stack.shape[0] // 4
    head = iota((rows, 128), 1) // HD
    out = jnp.zeros((rows, 128), stack.dtype)
    for j in range(4):
        out = jnp.where(head == j, stack[j * rows : (j + 1) * rows], out)
    return out


def halo_forward(points, places, occupieds, place, gains, table, w_qkv, w_out, w_up, w_down):
    unit, _ = normalise(points)
    normed = (unit * gains[0:1]).astype(BF)
    key_value = mm(normed, w_qkv[:, WIDTH:]).astype(BF)
    quarters = [slice(p * SLOTS + (3 - p) * QUAD, p * SLOTS + (4 - p) * QUAD) for p in range(4)]
    query = mm(jnp.concatenate([normed[r] for r in quarters], axis=0), w_qkv[:, :WIDTH]).astype(BF)
    hidden = jnp.concatenate([points[r] for r in quarters], axis=0)
    query_side = jnp.transpose(query_cells(place)).astype(BF)
    bias_left = mm(query_side, table_matrix(table)).astype(BF)
    key_sides = [
        jnp.transpose(key_cells(places[p], occupieds[p])).astype(BF) for p in range(4)
    ]
    scores, values = [], []
    for p in range(4):
        rows, window = slice(p * QUAD, (p + 1) * QUAD), slice(p * SLOTS, (p + 1) * SLOTS)
        for g in range(2):
            lanes = slice(128 * g, 128 * g + 128)
            k = key_value[window, 128 * g : 128 * g + 128]
            values.append(key_value[window, WIDTH + 128 * g : WIDTH + 128 * g + 128])
            lefts = jnp.concatenate(
                [bias_left[rows, 128 * h : 128 * h + 128] for h in range(4 * g, 4 * g + 4)], axis=0
            )
            scores.append(
                mm_t(
                    jnp.concatenate([spread(query[rows, lanes]), lefts], axis=1),
                    jnp.concatenate([k, key_sides[p]], axis=1),
                )
            )
    probs, mixed = attend(scores, values)
    mixed = [jnp.concatenate(mixed[2 * p : 2 * p + 2], axis=1) for p in range(4)]
    mixed = jnp.concatenate(mixed, axis=0)
    middle = hidden + mm(mixed.astype(BF), w_out[...])
    unit_two, inv_two = normalise(middle)
    up = mm((unit_two * gains[1:2]).astype(BF), w_up[...])
    expanded, slope = gelu_and_slope(up)
    out = middle + mm(expanded.astype(BF), w_down[...])
    return out.astype(BF), (key_value, probs, mixed, key_sides, unit_two, inv_two, slope)


def halo_table(cot, place, gains, saved, w_out, w_up, w_down):
    key_value, probs, mixed, key_sides, unit_two, inv_two, slope = saved
    _, cot_mixed = feed_forward_back(
        cot, gains, unit_two, inv_two, slope, w_out, w_up, w_down
    )
    cot_scores = []
    for p in range(4):
        rows, window = slice(p * QUAD, (p + 1) * QUAD), slice(p * SLOTS, (p + 1) * SLOTS)
        for g in range(2):
            lanes = slice(128 * g, 128 * g + 128)
            v = key_value[window, WIDTH + 128 * g : WIDTH + 128 * g + 128]
            cot_scores.append(
                attend_back(probs[2 * p + g], mixed[rows, lanes], cot_mixed[rows, lanes], v)
            )
    pair_rows = []
    for p in range(4):
        both = [mm(x, key_sides[p]) for x in cot_scores[2 * p : 2 * p + 2]]
        pair_rows.append(
            jnp.concatenate([x[j * QUAD : (j + 1) * QUAD] for x in both for j in range(4)], axis=1)
        )
    pairs = mm(cells(place, False).astype(BF), jnp.concatenate(pair_rows, axis=0).astype(BF))
    return table_sums(
        [
            [pairs[e * PITCH : e * PITCH + SPAN, 128 * h : 128 * h + 128] for e in range(3)]
            for h in range(HEADS)
        ]
    )


def pack_kernel(
    features, occupancy, coords, grad_out, to_y, to_x, to_xy, occupied, place, arrived
):
    pairs = [(occupancy, occupied), (coords, place)]
    for quarter, target in ((2, to_y), (1, to_x), (0, to_xy)):
        pairs.append((features, target.at[0:SLOTS]))
        rows = slice(quarter * QUAD, (quarter + 1) * QUAD)
        pairs.append((grad_out.at[rows], target.at[SLOTS : SLOTS + QUAD]))
    copies = [
        pltpu.make_async_copy(source, target, arrived.at[i])
        for i, (source, target) in enumerate(pairs)
    ]
    for copy in copies:
        copy.start()
    copies[0].wait()
    copies[1].wait()
    meta = jnp.concatenate(
        [occupied[...]] + [place[e] for e in range(3)] + [jnp.zeros((4, SLOTS), jnp.int32)], axis=0
    ).astype(F32)
    meta = jnp.concatenate([meta, jnp.zeros((8, SLOTS), F32)], axis=0)
    meta = jnp.concatenate([meta, jnp.zeros((16, SLOTS), F32)], axis=1).astype(BF)
    for target in (to_y, to_x, to_xy):
        target[SLOTS + QUAD :] = meta
    for copy in copies[2:]:
        copy.wait()


def main_kernel(
    features, occupancy, coords, grad_out, from_y, from_x, from_xy,
    gains, tables, w_qkv, w_out, w_up, w_down,
    own, back_y, back_x, back_xy, tables_out,
):
    received = (from_y, from_x, from_xy)
    points = jnp.concatenate(
        [features[...]] + [part[0:SLOTS] for part in received], axis=0
    ).astype(F32)
    grad = jnp.concatenate(
        [grad_out[3 * QUAD :]] + [part[SLOTS : SLOTS + QUAD] for part in received], axis=0
    )
    metas = [
        jnp.concatenate(
            [occupancy[...]] + [coords[e] for e in range(3)] + [jnp.zeros((4, SLOTS), jnp.int32)],
            axis=0,
        )
    ] + [
        part[SLOTS + QUAD :].astype(F32)[0:8, 0:SLOTS].astype(jnp.int32) for part in received
    ]
    quarter = iota((8, SLOTS), 1) // QUAD
    meta = jnp.zeros((8, SLOTS), jnp.int32)
    for position, part in enumerate(metas):
        moved = pltpu.roll(part, (2 * position - 3) * QUAD % SLOTS, 1)
        meta = jnp.where(quarter == position, moved, meta)
    occupied, place = meta[0:1], meta[1:4]
    half = SPAN // 2
    shifted = jnp.concatenate(
        [(place[0:1] + half) % SPAN, (place[1:2] + half) % SPAN, place[2:3]], axis=0
    )
    column = jnp.transpose(jnp.broadcast_to(occupied.astype(F32), (SLOTS, SLOTS)))
    grad = grad * jnp.concatenate([column, column], axis=1).astype(BF)
    first_weights = (w_qkv.at[0], w_out.at[0], w_up.at[0], w_down.at[0])
    second_weights = (w_qkv.at[1], w_out.at[1], w_up.at[1], w_down.at[1])
    first_out, first_saved = halo_forward(
        points, [m[1:4] for m in metas], [m[0:1] for m in metas], place, gains[0], tables[0],
        *first_weights,
    )
    hidden = first_out.astype(F32)
    second, second_saved = block_forward(
        hidden, gains[1], shifted, occupied, tables[1], *second_weights
    )
    cot, second_table = block_backward(
        grad, gains[1], shifted, second_saved, *second_weights
    )
    first_table = halo_table(cot, place, gains[0], first_saved, *first_weights[1:])
    for position, target in enumerate((own, back_y, back_x, back_xy)):
        rows = slice(position * QUAD, (position + 1) * QUAD)
        target[0:QUAD] = second[rows]
        target[QUAD:] = cot[rows]
    both = first_table + pltpu.roll(second_table, 3 * PITCH, 1)
    for i in range(tables_out.shape[0]):
        tables_out[i] = both.astype(BF)


def window_kernel(
    home_xy, home_x, home_y, own, features, occupancy, coords,
    gains, tables, w_qkv, w_out, w_up, w_down, out_points, grad_points,
):
    parts = (home_xy, home_x, home_y, own)
    second = jnp.concatenate([part[0:QUAD] for part in parts], axis=0)
    cot = jnp.concatenate([part[QUAD:] for part in parts], axis=0)
    column = jnp.transpose(jnp.broadcast_to(occupancy[...].astype(F32), (SLOTS, SLOTS)))
    out_points[...] = second * jnp.concatenate([column, column], axis=1).astype(BF)
    place = jnp.concatenate([coords[e] for e in range(3)], axis=0)
    weights = (w_qkv.at[0], w_out.at[0], w_up.at[0], w_down.at[0])
    points = features[...].astype(F32)
    _, saved = block_forward(points, gains[0], place, occupancy[...], tables[0], *weights)
    grad_points[...], _ = block_backward(
        cot, gains[0], place, saved, *weights, with_table=False
    )


def sum_of(parts):
    total = parts[0].astype(F32)
    for i in range(1, parts.shape[0]):
        total = total + parts[i].astype(F32)
    return total


def relay_kernel(parts, out):
    total = sum_of(parts).astype(BF)
    for i in range(out.shape[0]):
        out[i] = total


def unpack_kernel(parts, out):
    total = sum_of(parts)
    for k in range(2):
        for e in range(3):
            start = (3 * k + e) * PITCH
            moved = total if start == 0 else pltpu.roll(total, 128 - start, 1)
            out[k, e] = moved[:, : out.shape[-1]]


def call(kernel, shapes, *args, far=None, scratch=(), cost=None):
    options = {}
    if far is not None:
        args = args[:far] + tuple(in_hbm(a) for a in args[far:])
        options["in_specs"] = [pl.BlockSpec(memory_space=pl.ANY)] * far + [
            pl.BlockSpec(memory_space=pltpu.HBM)
        ] * (len(args) - far)
    return pl.pallas_call(
        kernel,
        out_shape=[jax.ShapeDtypeStruct(s, d) for s, d in shapes],
        scratch_shapes=scratch,
        compiler_params=pltpu.CompilerParams(vmem_limit_bytes=VMEM_LIMIT),
        cost_estimate=cost,
        interpret=INTERPRET,
        **options,
    )(*args)


def in_hbm(value):
    return value if INTERPRET else pltpu.with_memory_space_constraint(value, pltpu.HBM)


def on_device(
    gx, gy, phases,
    features, occupancy, coords, norm_gains, bias_tables, w_qkv, w_out, w_up, w_down, grad_out,
):
    size_x = lax.axis_size(gx)
    size_y = lax.axis_size(gy)

    def move(value, step_x, step_y):
        pairs = []
        for i in range(size_x):
            for j in range(size_y):
                target = (i + step_x) % size_x * size_y + (j + step_y) % size_y
                pairs.append((i * size_y + j, target))
        return lax.ppermute(value, gx + gy, pairs)

    points, occupied, grad = features[0, 0], occupancy[0], grad_out[0, 0]
    place = jnp.swapaxes(coords[0], 0, 1)
    packet, reply = ((SLOTS + QUAD + 16, WIDTH), BF), ((2 * QUAD, WIDTH), BF)
    to_y, to_x, to_xy = call(
        pack_kernel, [packet] * 3, points, occupied, place, grad, far=0,
        cost=pl.CostEstimate(flops=COST, transcendentals=0, bytes_accessed=8 * 1024 * 1024),
        scratch=[pltpu.VMEM(occupied.shape, jnp.int32), pltpu.VMEM(place.shape, jnp.int32), pltpu.SemaphoreType.DMA((8,))],
    )
    from_x = move(to_x, -1, 0)
    from_xy = move(to_xy, -1, -1)
    from_y = move(to_y, 0, -1)
    first = lax.axis_size(phases[0])
    staged = (points, occupied, place, grad, norm_gains, bias_tables, w_qkv, w_out, w_up, w_down)
    own, back_y, back_x, back_xy, tables = call(
        main_kernel,
        [reply] * 4 + [((first, HEADS, 128), BF)],
        *staged[:4], from_y, from_x, from_xy, *staged[4:],
    )
    home_y = move(back_y, 0, 1)
    home_x = move(back_x, 1, 0)
    home_xy = move(back_xy, 1, 1)
    tables = lax.all_to_all(tables, phases[0], 0, 0)
    (tables,) = call(relay_kernel, [((lax.axis_size(phases[1]), HEADS, 128), BF)], tables)
    tables = lax.all_to_all(tables, phases[1], 0, 0)
    (grad_tables,) = call(unpack_kernel, [(bias_tables.shape, F32)], tables)
    out_points, grad_points = call(
        window_kernel, [((SLOTS, WIDTH), BF)] * 2, home_xy, home_x, home_y, own, *staged[:3], *staged[4:]
    )
    return out_points[None, None], grad_points[None, None], grad_tables


def solution(mesh):
    shape = tuple(mesh.shape[a] for a in ("gx", "gy"))
    if shape == (16, 32):
        fine = Mesh(mesh.devices.reshape(2, 4, 2, 8, 4), ("zh", "y", "c", "zl", "x"))
        gx, gy = ("zh", "y", "c"), ("zl", "x")
        phases = (("zh", "zl"), ("y", "c", "x"))
    else:
        fine = Mesh(mesh.devices, ("gx", "gy"))
        gx, gy, phases = ("gx",), ("gy",), (("gx",), ("gy",))
    grid = P(gx, gy, None, None)
    return jax.shard_map(
        partial(on_device, gx, gy, phases),
        mesh=fine,
        in_specs=(grid, P(gx, gy, None), grid, P(), P(), P(), P(), P(), P(), grid),
        out_specs=(grid, grid, P()),
        check_vma=False,
    )
```

```python
from functools import partial

import jax
import jax.numpy as jnp
from jax import lax
from jax.experimental import pallas as pl
from jax.experimental.pallas import tpu as pltpu
from jax.sharding import Mesh
from jax.sharding import PartitionSpec as P

INTERPRET = False
EPS = 1e-05
BF = jnp.bfloat16
F32 = jnp.float32
SLOTS, WIDTH, HEADS, HD, QUAD = 128, 256, 8, 32, 32
SPAN, PITCH = 8, 16
SCALE = HD ** (-0.5)
MASKED = -1e30
COST = 10_000_000_000
VMEM_LIMIT = 24 * 1024 * 1024


def mm(a, b):
    return lax.dot_general(a, b, (((1,), (0,)), ((), ())), preferred_element_type=F32)


def mm_t(a, b):
    return lax.dot_general(a, b, (((1,), (1,)), ((), ())), preferred_element_type=F32)


def iota(shape, axis):
    return lax.broadcasted_iota(jnp.int32, shape, axis)


def normalise(values):
    centred = values - jnp.mean(values, axis=-1, keepdims=True)
    inv = lax.rsqrt(jnp.mean(centred * centred, axis=-1, keepdims=True) + EPS)
    return centred * inv, inv


def normalise_back(cot, unit, inv):
    return inv * (
        cot
        - jnp.mean(cot, axis=-1, keepdims=True)
        - unit * jnp.mean(cot * unit, axis=-1, keepdims=True)
    )


def cells(coords, mirrored):
    row = iota((PITCH, SLOTS), 0)
    if mirrored:
        row = SPAN - 1 - row
    return jnp.concatenate(
        [(coords[e : e + 1] == row).astype(F32) for e in range(3)], axis=0
    )


def query_cells(coords):
    ones = jnp.where(iota((PITCH, SLOTS), 0) == 0, 1.0, 0.0)
    return jnp.concatenate(
        [cells(coords, True), ones, jnp.zeros((SLOTS - 4 * PITCH, SLOTS), F32)], axis=0
    )


def key_cells(coords, occupied):
    mirrored = cells(coords, True)
    mask = jnp.where((iota((PITCH, SLOTS), 0) == 0) & (occupied <= 0), MASKED, 0.0)
    return jnp.concatenate([mirrored, mirrored, mask, jnp.zeros((PITCH, SLOTS), F32)], axis=0)


def table_matrix(table):
    lane = iota((SPAN, 128), 1)
    wide = []
    for e in range(3):
        row = jnp.concatenate(
            [table[e] * (1.0 / SCALE), jnp.zeros((HEADS, 128 - table.shape[-1]), F32)], axis=1
        )
        start = e * PITCH - (SPAN - 1)
        wide.append(
            pltpu.roll(row, start % 128, 1) + pltpu.roll(row, (start + 3 * PITCH) % 128, 1)
        )
    columns = []
    for h in range(HEADS):
        rows = []
        for e in range(3):
            value = pltpu.roll(
                jnp.broadcast_to(wide[e][h : h + 1], (SPAN, 128)), 0, 1, stride=1, stride_axis=0
            )
            high = value.astype(BF).astype(F32)
            value = jnp.where(lane < 3 * PITCH, high, value - high)
            base = lane % (3 * PITCH) - e * PITCH
            keep = (base >= 0) & (base < SPAN) & (lane < 6 * PITCH)
            rows += [jnp.where(keep, value, 0.0), jnp.zeros((SPAN, 128), F32)]
        one = (iota((PITCH, 128), 0) == 0) & (iota((PITCH, 128), 1) == 6 * PITCH)
        rows += [jnp.where(one, 1.0, 0.0), jnp.zeros((128 - 4 * PITCH, 128), F32)]
        columns.append(jnp.concatenate(rows, axis=0))
    return jnp.concatenate(columns, axis=1).astype(BF)


def spread(group):
    head = iota(group.shape, 1) // HD
    return jnp.concatenate(
        [jnp.where(head == j, group, jnp.zeros_like(group)) for j in range(4)], axis=0
    )


def side_by_side(stack):
    return jnp.concatenate([stack[j * SLOTS : (j + 1) * SLOTS] for j in range(4)], axis=1)


def attend(scores, values):
    tops = [jnp.max(x, axis=-1, keepdims=True) for x in scores]
    factor = SCALE * 1.4426950408889634
    weights = [jnp.exp2((x - top) * factor) for x, top in zip(scores, tops)]
    ones = jnp.ones_like(values[0])
    both = [mm(w.astype(BF), jnp.concatenate([v, ones], axis=1)) for w, v in zip(weights, values)]
    shares = [1.0 / x[:, 128:] for x in both]
    return (
        [w * share for w, share in zip(weights, shares)],
        [head_lanes(x[:, :128] * share) for x, share in zip(both, shares)],
    )


def attend_back(soft, mixed, cot_mixed, v):
    product = (-mixed * cot_mixed.astype(F32)).astype(BF)
    left = jnp.concatenate([spread(cot_mixed), spread(product)], axis=1)
    return (soft * mm_t(left, jnp.concatenate([v, jnp.ones_like(v)], axis=1))).astype(BF)


def gelu_and_slope(v):
    c = 0.7978845608028654
    square = v * v
    t = jnp.tanh(v * (c + (c * 0.044715) * square))
    half = 0.5 + 0.5 * t
    return v * half, half + (0.5 * v) * (1.0 - t * t) * (c + (3 * c * 0.044715) * square)


def block_forward(hidden, gains, coords, occupied, table, w_qkv, w_out, w_up, w_down):
    unit, inv = normalise(hidden)
    projected = mm((unit * gains[0:1]).astype(BF), w_qkv[...]).astype(BF)
    query_side = jnp.transpose(query_cells(coords)).astype(BF)
    key_side = jnp.transpose(key_cells(coords, occupied)).astype(BF)
    bias_left = mm(query_side, table_matrix(table)).astype(BF)
    scores, values = [], []
    for g in range(2):
        q = projected[:, 128 * g : 128 * g + 128]
        k = projected[:, 256 + 128 * g : 256 + 128 * g + 128]
        values.append(projected[:, 512 + 128 * g : 512 + 128 * g + 128])
        lefts = jnp.concatenate(
            [bias_left[:, 128 * h : 128 * h + 128] for h in range(4 * g, 4 * g + 4)], axis=0
        )
        scores.append(
            mm_t(jnp.concatenate([spread(q), lefts], axis=1), jnp.concatenate([k, key_side], axis=1))
        )
    probs, mixed = attend(scores, values)
    mixed = jnp.concatenate(mixed, axis=1)
    middle = hidden + mm(mixed.astype(BF), w_out[...])
    unit_two, inv_two = normalise(middle)
    up = mm((unit_two * gains[1:2]).astype(BF), w_up[...])
    expanded, slope = gelu_and_slope(up)
    out = middle + mm(expanded.astype(BF), w_down[...])
    return out.astype(BF), (projected, probs, mixed, unit, inv, unit_two, inv_two, slope)


def feed_forward_back(cot, gains, unit, inv, slope, w_out, w_up, w_down):
    cot_up = mm_t(cot, w_down[...]) * slope
    cot_two = mm_t(cot_up.astype(BF), w_up[...]) * gains[1:2]
    cot_middle = cot.astype(F32) + normalise_back(cot_two, unit, inv)
    return cot_middle, mm_t(cot_middle.astype(BF), w_out[...]).astype(BF)


def table_sums(per_head):
    lane = iota((SPAN, 128), 1)
    tables = []
    for blocks in per_head:
        value = jnp.where(lane < PITCH, blocks[0], jnp.where(lane < 2 * PITCH, blocks[1], blocks[2]))
        value = jnp.where(lane < 3 * PITCH, value, 0.0)
        value = pltpu.roll(value, 0, 1, stride=1, stride_axis=0)
        tables.append(jnp.sum(value, axis=0, keepdims=True))
    return jnp.concatenate(tables, axis=0)


def block_backward(cot, gains, coords, saved, w_qkv, w_out, w_up, w_down, with_table=True):
    projected, probs, mixed, unit, inv, unit_two, inv_two, slope = saved
    cot_middle, cot_mixed = feed_forward_back(
        cot, gains, unit_two, inv_two, slope, w_out, w_up, w_down
    )
    cells_t = cells(coords, False).astype(BF)
    blank = jnp.zeros((SLOTS - 3 * PITCH, SLOTS), F32)
    cells_key = jnp.transpose(jnp.concatenate([cells(coords, True), blank], axis=0)).astype(BF)
    cot_q, cot_k, cot_v, pair_sums = [], [], [], []
    for g in range(2):
        q = projected[:, 128 * g : 128 * g + 128]
        k = projected[:, 256 + 128 * g : 256 + 128 * g + 128]
        v = projected[:, 512 + 128 * g : 512 + 128 * g + 128]
        dm = cot_mixed[:, 128 * g : 128 * g + 128]
        q_t = jnp.transpose(q.astype(F32)).astype(BF)
        dm_t = jnp.transpose(dm.astype(F32)).astype(BF)
        cot_scores = attend_back(probs[g], mixed[:, 128 * g : 128 * g + 128], dm, v)
        soft = probs[g].astype(BF)
        cot_q.append(mm(side_by_side(cot_scores), spread(k)) * SCALE)
        k_rows, v_rows = [], []
        for j in range(4):
            rows = slice(j * SLOTS, (j + 1) * SLOTS)
            lanes = slice(j * HD, (j + 1) * HD)
            left = jnp.concatenate([q_t[lanes], cells_t], axis=0) if with_table else q_t[lanes]
            both = mm(left, cot_scores[rows])
            k_rows.append(both[:HD])
            pair_sums.append(both[HD:])
            v_rows.append(mm(dm_t[lanes], soft[rows]))
        cot_k.append(jnp.transpose(jnp.concatenate(k_rows, axis=0)) * SCALE)
        cot_v.append(jnp.transpose(jnp.concatenate(v_rows, axis=0)))
    cot_projected = jnp.concatenate(cot_q + cot_k + cot_v, axis=1).astype(BF)
    cot_normed = mm_t(cot_projected, w_qkv[...]) * gains[0:1]
    cot_hidden = cot_middle + normalise_back(cot_normed, unit, inv)
    if not with_table:
        return cot_hidden.astype(BF), None
    pairs = mm(jnp.concatenate(pair_sums, axis=0).astype(BF), cells_key)
    per_head = [
        [pairs[(3 * h + e) * PITCH : (3 * h + e) * PITCH + SPAN] for e in range(3)]
        for h in range(HEADS)
    ]
    return cot_hidden.astype(BF), table_sums(per_head)


def head_lanes(stack):
    rows = stack.shape[0] // 4
    head = iota((rows, 128), 1) // HD
    out = jnp.zeros((rows, 128), stack.dtype)
    for j in range(4):
        out = jnp.where(head == j, stack[j * rows : (j + 1) * rows], out)
    return out


def halo_forward(points, places, occupieds, place, gains, table, w_qkv, w_out, w_up, w_down):
    unit, _ = normalise(points)
    normed = (unit * gains[0:1]).astype(BF)
    key_value = mm(normed, w_qkv[:, WIDTH:]).astype(BF)
    quarters = [slice(p * SLOTS + (3 - p) * QUAD, p * SLOTS + (4 - p) * QUAD) for p in range(4)]
    query = mm(jnp.concatenate([normed[r] for r in quarters], axis=0), w_qkv[:, :WIDTH]).astype(BF)
    hidden = jnp.concatenate([points[r] for r in quarters], axis=0)
    query_side = jnp.transpose(query_cells(place)).astype(BF)
    bias_left = mm(query_side, table_matrix(table)).astype(BF)
    key_sides = [
        jnp.transpose(key_cells(places[p], occupieds[p])).astype(BF) for p in range(4)
    ]
    scores, values = [], []
    for p in range(4):
        rows, window = slice(p * QUAD, (p + 1) * QUAD), slice(p * SLOTS, (p + 1) * SLOTS)
        for g in range(2):
            lanes = slice(128 * g, 128 * g + 128)
            k = key_value[window, 128 * g : 128 * g + 128]
            values.append(key_value[window, WIDTH + 128 * g : WIDTH + 128 * g + 128])
            lefts = jnp.concatenate(
                [bias_left[rows, 128 * h : 128 * h + 128] for h in range(4 * g, 4 * g + 4)], axis=0
            )
            scores.append(
                mm_t(
                    jnp.concatenate([spread(query[rows, lanes]), lefts], axis=1),
                    jnp.concatenate([k, key_sides[p]], axis=1),
                )
            )
    probs, mixed = attend(scores, values)
    mixed = [jnp.concatenate(mixed[2 * p : 2 * p + 2], axis=1) for p in range(4)]
    mixed = jnp.concatenate(mixed, axis=0)
    middle = hidden + mm(mixed.astype(BF), w_out[...])
    unit_two, inv_two = normalise(middle)
    up = mm((unit_two * gains[1:2]).astype(BF), w_up[...])
    expanded, slope = gelu_and_slope(up)
    out = middle + mm(expanded.astype(BF), w_down[...])
    return out.astype(BF), (key_value, probs, mixed, key_sides, unit_two, inv_two, slope)


def halo_table(cot, place, gains, saved, w_out, w_up, w_down):
    key_value, probs, mixed, key_sides, unit_two, inv_two, slope = saved
    _, cot_mixed = feed_forward_back(
        cot, gains, unit_two, inv_two, slope, w_out, w_up, w_down
    )
    cot_scores = []
    for p in range(4):
        rows, window = slice(p * QUAD, (p + 1) * QUAD), slice(p * SLOTS, (p + 1) * SLOTS)
        for g in range(2):
            lanes = slice(128 * g, 128 * g + 128)
            v = key_value[window, WIDTH + 128 * g : WIDTH + 128 * g + 128]
            cot_scores.append(
                attend_back(probs[2 * p + g], mixed[rows, lanes], cot_mixed[rows, lanes], v)
            )
    pair_rows = []
    for p in range(4):
        both = [mm(x, key_sides[p]) for x in cot_scores[2 * p : 2 * p + 2]]
        pair_rows.append(
            jnp.concatenate([x[j * QUAD : (j + 1) * QUAD] for x in both for j in range(4)], axis=1)
        )
    pairs = mm(cells(place, False).astype(BF), jnp.concatenate(pair_rows, axis=0).astype(BF))
    return table_sums(
        [
            [pairs[e * PITCH : e * PITCH + SPAN, 128 * h : 128 * h + 128] for e in range(3)]
            for h in range(HEADS)
        ]
    )


def pack_kernel(
    features, occupancy, coords, grad_out, to_y, to_x, to_xy, occupied, place, arrived
):
    pairs = [(occupancy, occupied), (coords, place)]
    for quarter, target in ((2, to_y), (1, to_x), (0, to_xy)):
        pairs.append((features, target.at[0:SLOTS]))
        rows = slice(quarter * QUAD, (quarter + 1) * QUAD)
        pairs.append((grad_out.at[rows], target.at[SLOTS : SLOTS + QUAD]))
    copies = [
        pltpu.make_async_copy(source, target, arrived.at[i])
        for i, (source, target) in enumerate(pairs)
    ]
    for copy in copies:
        copy.start()
    copies[0].wait()
    copies[1].wait()
    meta = jnp.concatenate(
        [occupied[...]] + [place[e] for e in range(3)] + [jnp.zeros((4, SLOTS), jnp.int32)], axis=0
    ).astype(F32)
    meta = jnp.concatenate([meta, jnp.zeros((8, SLOTS), F32)], axis=1).astype(BF)
    for target in (to_y, to_x, to_xy):
        target[SLOTS + QUAD :] = meta
    for copy in copies[2:]:
        copy.wait()


def main_kernel(
    features, occupancy, coords, grad_out, from_y, from_x, from_xy,
    gains, tables, w_qkv, w_out, w_up, w_down,
    own, back_y, back_x, back_xy, tables_out,
):
    received = (from_y, from_x, from_xy)
    points = jnp.concatenate(
        [features[...]] + [part[0:SLOTS] for part in received], axis=0
    ).astype(F32)
    grad = jnp.concatenate(
        [grad_out[3 * QUAD :]] + [part[SLOTS : SLOTS + QUAD] for part in received], axis=0
    )
    metas = [
        jnp.concatenate(
            [occupancy[...]] + [coords[e] for e in range(3)] + [jnp.zeros((4, SLOTS), jnp.int32)],
            axis=0,
        )
    ] + [
        part[SLOTS + QUAD :].astype(F32)[:, 0:SLOTS].astype(jnp.int32) for part in received
    ]
    quarter = iota((8, SLOTS), 1) // QUAD
    meta = jnp.zeros((8, SLOTS), jnp.int32)
    for position, part in enumerate(metas):
        moved = pltpu.roll(part, (2 * position - 3) * QUAD % SLOTS, 1)
        meta = jnp.where(quarter == position, moved, meta)
    occupied, place = meta[0:1], meta[1:4]
    half = SPAN // 2
    shifted = jnp.concatenate(
        [(place[0:1] + half) % SPAN, (place[1:2] + half) % SPAN, place[2:3]], axis=0
    )
    column = jnp.transpose(jnp.broadcast_to(occupied.astype(F32), (SLOTS, SLOTS)))
    grad = grad * jnp.concatenate([column, column], axis=1).astype(BF)
    first_weights = (w_qkv.at[0], w_out.at[0], w_up.at[0], w_down.at[0])
    second_weights = (w_qkv.at[1], w_out.at[1], w_up.at[1], w_down.at[1])
    first_out, first_saved = halo_forward(
        points, [m[1:4] for m in metas], [m[0:1] for m in metas], place, gains[0], tables[0],
        *first_weights,
    )
    hidden = first_out.astype(F32)
    second, second_saved = block_forward(
        hidden, gains[1], shifted, occupied, tables[1], *second_weights
    )
    cot, second_table = block_backward(
        grad, gains[1], shifted, second_saved, *second_weights
    )
    first_table = halo_table(cot, place, gains[0], first_saved, *first_weights[1:])
    for position, target in enumerate((own, back_y, back_x, back_xy)):
        rows = slice(position * QUAD, (position + 1) * QUAD)
        target[0:QUAD] = second[rows]
        target[QUAD:] = cot[rows]
    both = first_table + pltpu.roll(second_table, 3 * PITCH, 1)
    for i in range(tables_out.shape[0]):
        tables_out[i] = both.astype(BF)


def window_kernel(
    home_xy, home_x, home_y, own, features, occupancy, coords,
    gains, tables, w_qkv, w_out, w_up, w_down, out_points, grad_points,
):
    parts = (home_xy, home_x, home_y, own)
    second = jnp.concatenate([part[0:QUAD] for part in parts], axis=0)
    cot = jnp.concatenate([part[QUAD:] for part in parts], axis=0)
    column = jnp.transpose(jnp.broadcast_to(occupancy[...].astype(F32), (SLOTS, SLOTS)))
    out_points[...] = second * jnp.concatenate([column, column], axis=1).astype(BF)
    place = jnp.concatenate([coords[e] for e in range(3)], axis=0)
    weights = (w_qkv.at[0], w_out.at[0], w_up.at[0], w_down.at[0])
    points = features[...].astype(F32)
    _, saved = block_forward(points, gains[0], place, occupancy[...], tables[0], *weights)
    grad_points[...], _ = block_backward(
        cot, gains[0], place, saved, *weights, with_table=False
    )


def sum_of(parts):
    total = parts[0].astype(F32)
    for i in range(1, parts.shape[0]):
        total = total + parts[i].astype(F32)
    return total


def relay_kernel(parts, out):
    total = sum_of(parts).astype(BF)
    for i in range(out.shape[0]):
        out[i] = total


def unpack_kernel(parts, out):
    total = sum_of(parts)
    for k in range(2):
        for e in range(3):
            start = (3 * k + e) * PITCH
            moved = total if start == 0 else pltpu.roll(total, 128 - start, 1)
            out[k, e] = moved[:, : out.shape[-1]]


def call(kernel, shapes, *args, far=None, scratch=(), cost=None):
    options = {}
    if far is not None:
        args = args[:far] + tuple(in_hbm(a) for a in args[far:])
        options["in_specs"] = [pl.BlockSpec(memory_space=pl.ANY)] * far + [
            pl.BlockSpec(memory_space=pltpu.HBM)
        ] * (len(args) - far)
    return pl.pallas_call(
        kernel,
        out_shape=[jax.ShapeDtypeStruct(s, d) for s, d in shapes],
        scratch_shapes=scratch,
        compiler_params=pltpu.CompilerParams(vmem_limit_bytes=VMEM_LIMIT),
        cost_estimate=cost,
        interpret=INTERPRET,
        **options,
    )(*args)


def in_hbm(value):
    return value if INTERPRET else pltpu.with_memory_space_constraint(value, pltpu.HBM)


def on_device(
    gx, gy, phases,
    features, occupancy, coords, norm_gains, bias_tables, w_qkv, w_out, w_up, w_down, grad_out,
):
    size_x = lax.axis_size(gx)
    size_y = lax.axis_size(gy)

    def move(value, step_x, step_y):
        pairs = []
        for i in range(size_x):
            for j in range(size_y):
                target = (i + step_x) % size_x * size_y + (j + step_y) % size_y
                pairs.append((i * size_y + j, target))
        return lax.ppermute(value, gx + gy, pairs)

    points, occupied, grad = features[0, 0], occupancy[0], grad_out[0, 0]
    place = jnp.swapaxes(coords[0], 0, 1)
    packet, reply = ((SLOTS + QUAD + 8, WIDTH), BF), ((2 * QUAD, WIDTH), BF)
    to_y, to_x, to_xy = call(
        pack_kernel, [packet] * 3, points, occupied, place, grad, far=0,
        cost=pl.CostEstimate(flops=COST, transcendentals=0, bytes_accessed=8 * 1024 * 1024),
        scratch=[pltpu.VMEM(occupied.shape, jnp.int32), pltpu.VMEM(place.shape, jnp.int32), pltpu.SemaphoreType.DMA((8,))],
    )
    from_x = move(to_x, -1, 0)
    from_xy = move(to_xy, -1, -1)
    from_y = move(to_y, 0, -1)
    first = lax.axis_size(phases[0])
    staged = (points, occupied, place, grad, norm_gains, bias_tables, w_qkv, w_out, w_up, w_down)
    own, back_y, back_x, back_xy, tables = call(
        main_kernel,
        [reply] * 4 + [((first, HEADS, 128), BF)],
        *staged[:4], from_y, from_x, from_xy, *staged[4:],
    )
    home_y = move(back_y, 0, 1)
    home_x = move(back_x, 1, 0)
    home_xy = move(back_xy, 1, 1)
    tables = lax.all_to_all(tables, phases[0], 0, 0)
    (tables,) = call(relay_kernel, [((lax.axis_size(phases[1]), HEADS, 128), BF)], tables)
    tables = lax.all_to_all(tables, phases[1], 0, 0)
    (grad_tables,) = call(unpack_kernel, [(bias_tables.shape, F32)], tables)
    out_points, grad_points = call(
        window_kernel, [((SLOTS, WIDTH), BF)] * 2, home_xy, home_x, home_y, own, *staged[:3], *staged[4:]
    )
    return out_points[None, None], grad_points[None, None], grad_tables


def solution(mesh):
    shape = tuple(mesh.shape[a] for a in ("gx", "gy"))
    if shape == (16, 32):
        fine = Mesh(mesh.devices.reshape(2, 4, 2, 8, 4), ("zh", "y", "c", "zl", "x"))
        gx, gy = ("zh", "y", "c"), ("zl", "x")
        phases = (("zh", "zl"), ("y", "c", "x"))
    else:
        fine = Mesh(mesh.devices, ("gx", "gy"))
        gx, gy, phases = ("gx",), ("gy",), (("gx",), ("gy",))
    grid = P(gx, gy, None, None)
    return jax.shard_map(
        partial(on_device, gx, gy, phases),
        mesh=fine,
        in_specs=(grid, P(gx, gy, None), grid, P(), P(), P(), P(), P(), P(), grid),
        out_specs=(grid, grid, P()),
        check_vma=False,
    )
```

```python
from functools import partial

import jax
import jax.numpy as jnp
from jax import lax
from jax.experimental import pallas as pl
from jax.experimental.pallas import tpu as pltpu
from jax.sharding import Mesh
from jax.sharding import PartitionSpec as P

INTERPRET = False
EPS = 1e-05
BF = jnp.bfloat16
F32 = jnp.float32
SLOTS, WIDTH, HEADS, HD, QUAD = 128, 256, 8, 32, 32
SPAN, PITCH = 8, 16
SCALE = HD ** (-0.5)
MASKED = -1e30
COST = 10_000_000_000
VMEM_LIMIT = 24 * 1024 * 1024


def mm(a, b):
    return lax.dot_general(a, b, (((1,), (0,)), ((), ())), preferred_element_type=F32)


def mm_t(a, b):
    return lax.dot_general(a, b, (((1,), (1,)), ((), ())), preferred_element_type=F32)


def iota(shape, axis):
    return lax.broadcasted_iota(jnp.int32, shape, axis)


def normalise(values):
    centred = values - jnp.mean(values, axis=-1, keepdims=True)
    inv = lax.rsqrt(jnp.mean(centred * centred, axis=-1, keepdims=True) + EPS)
    return centred * inv, inv


def normalise_back(cot, unit, inv):
    return inv * (
        cot
        - jnp.mean(cot, axis=-1, keepdims=True)
        - unit * jnp.mean(cot * unit, axis=-1, keepdims=True)
    )


def cells(coords, mirrored):
    row = iota((PITCH, SLOTS), 0)
    if mirrored:
        row = SPAN - 1 - row
    return jnp.concatenate(
        [(coords[e : e + 1] == row).astype(F32) for e in range(3)], axis=0
    )


def query_cells(coords):
    ones = jnp.where(iota((PITCH, SLOTS), 0) == 0, 1.0, 0.0)
    return jnp.concatenate(
        [cells(coords, True), ones, jnp.zeros((SLOTS - 4 * PITCH, SLOTS), F32)], axis=0
    )


def key_cells(coords, occupied):
    mirrored = cells(coords, True)
    mask = jnp.where((iota((PITCH, SLOTS), 0) == 0) & (occupied <= 0), MASKED, 0.0)
    return jnp.concatenate([mirrored, mirrored, mask, jnp.zeros((PITCH, SLOTS), F32)], axis=0)


def table_matrix(table):
    lane = iota((SPAN, 128), 1)
    wide = []
    for e in range(3):
        row = jnp.concatenate(
            [table[e] * (1.0 / SCALE), jnp.zeros((HEADS, 128 - table.shape[-1]), F32)], axis=1
        )
        start = e * PITCH - (SPAN - 1)
        wide.append(
            pltpu.roll(row, start % 128, 1) + pltpu.roll(row, (start + 3 * PITCH) % 128, 1)
        )
    columns = []
    for h in range(HEADS):
        rows = []
        for e in range(3):
            value = pltpu.roll(
                jnp.broadcast_to(wide[e][h : h + 1], (SPAN, 128)), 0, 1, stride=1, stride_axis=0
            )
            high = value.astype(BF).astype(F32)
            value = jnp.where(lane < 3 * PITCH, high, value - high)
            base = lane % (3 * PITCH) - e * PITCH
            keep = (base >= 0) & (base < SPAN) & (lane < 6 * PITCH)
            rows += [jnp.where(keep, value, 0.0), jnp.zeros((SPAN, 128), F32)]
        one = (iota((PITCH, 128), 0) == 0) & (iota((PITCH, 128), 1) == 6 * PITCH)
        rows += [jnp.where(one, 1.0, 0.0), jnp.zeros((128 - 4 * PITCH, 128), F32)]
        columns.append(jnp.concatenate(rows, axis=0))
    return jnp.concatenate(columns, axis=1).astype(BF)


def spread(group):
    head = iota(group.shape, 1) // HD
    return jnp.concatenate(
        [jnp.where(head == j, group, jnp.zeros_like(group)) for j in range(4)], axis=0
    )


def side_by_side(stack):
    return jnp.concatenate([stack[j * SLOTS : (j + 1) * SLOTS] for j in range(4)], axis=1)


def attend(scores, values):
    tops = [jnp.max(x, axis=-1, keepdims=True) for x in scores]
    factor = SCALE * 1.4426950408889634
    weights = [jnp.exp2((x - top) * factor) for x, top in zip(scores, tops)]
    ones = jnp.ones_like(values[0])
    both = [mm(w.astype(BF), jnp.concatenate([v, ones], axis=1)) for w, v in zip(weights, values)]
    shares = [1.0 / x[:, 128:] for x in both]
    return (
        [w * share for w, share in zip(weights, shares)],
        [head_lanes(x[:, :128] * share) for x, share in zip(both, shares)],
    )


def attend_back(soft, mixed, cot_mixed, v):
    product = -mixed * cot_mixed.astype(F32)
    high = product.astype(BF)
    low = (product - high.astype(F32)).astype(BF)
    ones = jnp.ones_like(v)
    left = jnp.concatenate([spread(cot_mixed), spread(high), spread(low)], axis=1)
    return (soft * mm_t(left, jnp.concatenate([v, ones, ones], axis=1))).astype(BF)


def gelu_and_slope(v):
    c = 0.7978845608028654
    square = v * v
    t = jnp.tanh(v * (c + (c * 0.044715) * square))
    half = 0.5 + 0.5 * t
    return v * half, half + (0.5 * v) * (1.0 - t * t) * (c + (3 * c * 0.044715) * square)


def block_forward(hidden, gains, coords, occupied, table, w_qkv, w_out, w_up, w_down):
    unit, inv = normalise(hidden)
    projected = mm((unit * gains[0:1]).astype(BF), w_qkv[...]).astype(BF)
    query_side = jnp.transpose(query_cells(coords)).astype(BF)
    key_side = jnp.transpose(key_cells(coords, occupied)).astype(BF)
    bias_left = mm(query_side, table_matrix(table)).astype(BF)
    scores, values = [], []
    for g in range(2):
        q = projected[:, 128 * g : 128 * g + 128]
        k = projected[:, 256 + 128 * g : 256 + 128 * g + 128]
        values.append(projected[:, 512 + 128 * g : 512 + 128 * g + 128])
        lefts = jnp.concatenate(
            [bias_left[:, 128 * h : 128 * h + 128] for h in range(4 * g, 4 * g + 4)], axis=0
        )
        scores.append(
            mm_t(jnp.concatenate([spread(q), lefts], axis=1), jnp.concatenate([k, key_side], axis=1))
        )
    probs, mixed = attend(scores, values)
    mixed = jnp.concatenate(mixed, axis=1)
    middle = hidden + mm(mixed.astype(BF), w_out[...])
    unit_two, inv_two = normalise(middle)
    up = mm((unit_two * gains[1:2]).astype(BF), w_up[...])
    expanded, slope = gelu_and_slope(up)
    out = middle + mm(expanded.astype(BF), w_down[...])
    return out.astype(BF), (projected, probs, mixed, unit, inv, unit_two, inv_two, slope)


def feed_forward_back(cot, gains, unit, inv, slope, w_out, w_up, w_down):
    cot_up = mm_t(cot, w_down[...]) * slope
    cot_two = mm_t(cot_up.astype(BF), w_up[...]) * gains[1:2]
    cot_middle = cot.astype(F32) + normalise_back(cot_two, unit, inv)
    return cot_middle, mm_t(cot_middle.astype(BF), w_out[...]).astype(BF)


def table_sums(per_head):
    lane = iota((SPAN, 128), 1)
    tables = []
    for blocks in per_head:
        value = jnp.where(lane < PITCH, blocks[0], jnp.where(lane < 2 * PITCH, blocks[1], blocks[2]))
        value = jnp.where(lane < 3 * PITCH, value, 0.0)
        value = pltpu.roll(value, 0, 1, stride=1, stride_axis=0)
        tables.append(jnp.sum(value, axis=0, keepdims=True))
    return jnp.concatenate(tables, axis=0)


def block_backward(cot, gains, coords, saved, w_qkv, w_out, w_up, w_down, with_table=True):
    projected, probs, mixed, unit, inv, unit_two, inv_two, slope = saved
    cot_middle, cot_mixed = feed_forward_back(
        cot, gains, unit_two, inv_two, slope, w_out, w_up, w_down
    )
    cells_t = cells(coords, False).astype(BF)
    blank = jnp.zeros((SLOTS - 3 * PITCH, SLOTS), F32)
    cells_key = jnp.transpose(jnp.concatenate([cells(coords, True), blank], axis=0)).astype(BF)
    cot_q, cot_k, cot_v, pair_sums = [], [], [], []
    for g in range(2):
        q = projected[:, 128 * g : 128 * g + 128]
        k = projected[:, 256 + 128 * g : 256 + 128 * g + 128]
        v = projected[:, 512 + 128 * g : 512 + 128 * g + 128]
        dm = cot_mixed[:, 128 * g : 128 * g + 128]
        q_t = jnp.transpose(q.astype(F32)).astype(BF)
        dm_t = jnp.transpose(dm.astype(F32)).astype(BF)
        cot_scores = attend_back(probs[g], mixed[:, 128 * g : 128 * g + 128], dm, v)
        soft = probs[g].astype(BF)
        cot_q.append(mm(side_by_side(cot_scores), spread(k)) * SCALE)
        k_rows, v_rows = [], []
        for j in range(4):
            rows = slice(j * SLOTS, (j + 1) * SLOTS)
            lanes = slice(j * HD, (j + 1) * HD)
            left = jnp.concatenate([q_t[lanes], cells_t], axis=0) if with_table else q_t[lanes]
            both = mm(left, cot_scores[rows])
            k_rows.append(both[:HD])
            pair_sums.append(both[HD:])
            v_rows.append(mm(dm_t[lanes], soft[rows]))
        cot_k.append(jnp.transpose(jnp.concatenate(k_rows, axis=0)) * SCALE)
        cot_v.append(jnp.transpose(jnp.concatenate(v_rows, axis=0)))
    cot_projected = jnp.concatenate(cot_q + cot_k + cot_v, axis=1).astype(BF)
    cot_normed = mm_t(cot_projected, w_qkv[...]) * gains[0:1]
    cot_hidden = cot_middle + normalise_back(cot_normed, unit, inv)
    if not with_table:
        return cot_hidden.astype(BF), None
    pairs = mm(jnp.concatenate(pair_sums, axis=0).astype(BF), cells_key)
    per_head = [
        [pairs[(3 * h + e) * PITCH : (3 * h + e) * PITCH + SPAN] for e in range(3)]
        for h in range(HEADS)
    ]
    return cot_hidden.astype(BF), table_sums(per_head)


def head_lanes(stack):
    rows = stack.shape[0] // 4
    head = iota((rows, 128), 1) // HD
    out = jnp.zeros((rows, 128), stack.dtype)
    for j in range(4):
        out = jnp.where(head == j, stack[j * rows : (j + 1) * rows], out)
    return out


def halo_forward(points, places, occupieds, place, gains, table, w_qkv, w_out, w_up, w_down):
    unit, _ = normalise(points)
    normed = (unit * gains[0:1]).astype(BF)
    key_value = mm(normed, w_qkv[:, WIDTH:]).astype(BF)
    quarters = [slice(p * SLOTS + (3 - p) * QUAD, p * SLOTS + (4 - p) * QUAD) for p in range(4)]
    query = mm(jnp.concatenate([normed[r] for r in quarters], axis=0), w_qkv[:, :WIDTH]).astype(BF)
    hidden = jnp.concatenate([points[r] for r in quarters], axis=0)
    query_side = jnp.transpose(query_cells(place)).astype(BF)
    bias_left = mm(query_side, table_matrix(table)).astype(BF)
    key_sides = [
        jnp.transpose(key_cells(places[p], occupieds[p])).astype(BF) for p in range(4)
    ]
    scores, values = [], []
    for p in range(4):
        rows, window = slice(p * QUAD, (p + 1) * QUAD), slice(p * SLOTS, (p + 1) * SLOTS)
        for g in range(2):
            lanes = slice(128 * g, 128 * g + 128)
            k = key_value[window, 128 * g : 128 * g + 128]
            values.append(key_value[window, WIDTH + 128 * g : WIDTH + 128 * g + 128])
            lefts = jnp.concatenate(
                [bias_left[rows, 128 * h : 128 * h + 128] for h in range(4 * g, 4 * g + 4)], axis=0
            )
            scores.append(
                mm_t(
                    jnp.concatenate([spread(query[rows, lanes]), lefts], axis=1),
                    jnp.concatenate([k, key_sides[p]], axis=1),
                )
            )
    probs, mixed = attend(scores, values)
    mixed = [jnp.concatenate(mixed[2 * p : 2 * p + 2], axis=1) for p in range(4)]
    mixed = jnp.concatenate(mixed, axis=0)
    middle = hidden + mm(mixed.astype(BF), w_out[...])
    unit_two, inv_two = normalise(middle)
    up = mm((unit_two * gains[1:2]).astype(BF), w_up[...])
    expanded, slope = gelu_and_slope(up)
    out = middle + mm(expanded.astype(BF), w_down[...])
    return out.astype(BF), (key_value, probs, mixed, key_sides, unit_two, inv_two, slope)


def halo_table(cot, place, gains, saved, w_out, w_up, w_down):
    key_value, probs, mixed, key_sides, unit_two, inv_two, slope = saved
    _, cot_mixed = feed_forward_back(
        cot, gains, unit_two, inv_two, slope, w_out, w_up, w_down
    )
    cot_scores = []
    for p in range(4):
        rows, window = slice(p * QUAD, (p + 1) * QUAD), slice(p * SLOTS, (p + 1) * SLOTS)
        for g in range(2):
            lanes = slice(128 * g, 128 * g + 128)
            v = key_value[window, WIDTH + 128 * g : WIDTH + 128 * g + 128]
            cot_scores.append(
                attend_back(probs[2 * p + g], mixed[rows, lanes], cot_mixed[rows, lanes], v)
            )
    pair_rows = []
    for p in range(4):
        both = [mm(x, key_sides[p]) for x in cot_scores[2 * p : 2 * p + 2]]
        pair_rows.append(
            jnp.concatenate([x[j * QUAD : (j + 1) * QUAD] for x in both for j in range(4)], axis=1)
        )
    pairs = mm(cells(place, False).astype(BF), jnp.concatenate(pair_rows, axis=0).astype(BF))
    return table_sums(
        [
            [pairs[e * PITCH : e * PITCH + SPAN, 128 * h : 128 * h + 128] for e in range(3)]
            for h in range(HEADS)
        ]
    )


def pack_kernel(
    features, occupancy, coords, grad_out, to_y, to_x, to_xy, occupied, place, arrived
):
    pairs = [(occupancy, occupied), (coords, place)]
    for quarter, target in ((2, to_y), (1, to_x), (0, to_xy)):
        pairs.append((features, target.at[0:SLOTS]))
        rows = slice(quarter * QUAD, (quarter + 1) * QUAD)
        pairs.append((grad_out.at[rows], target.at[SLOTS : SLOTS + QUAD]))
    copies = [
        pltpu.make_async_copy(source, target, arrived.at[i])
        for i, (source, target) in enumerate(pairs)
    ]
    for copy in copies:
        copy.start()
    copies[0].wait()
    copies[1].wait()
    meta = jnp.concatenate(
        [occupied[...]] + [place[e] for e in range(3)] + [jnp.zeros((4, SLOTS), jnp.int32)], axis=0
    ).astype(F32)
    meta = jnp.concatenate([meta, jnp.zeros((8, SLOTS), F32)], axis=1).astype(BF)
    for target in (to_y, to_x, to_xy):
        target[SLOTS + QUAD :] = meta
    for copy in copies[2:]:
        copy.wait()


def main_kernel(
    features, occupancy, coords, grad_out, from_y, from_x, from_xy,
    gains, tables, w_qkv, w_out, w_up, w_down,
    own, back_y, back_x, back_xy, tables_out,
):
    received = (from_y, from_x, from_xy)
    points = jnp.concatenate(
        [features[...]] + [part[0:SLOTS] for part in received], axis=0
    ).astype(F32)
    grad = jnp.concatenate(
        [grad_out[3 * QUAD :]] + [part[SLOTS : SLOTS + QUAD] for part in received], axis=0
    )
    metas = [
        jnp.concatenate(
            [occupancy[...]] + [coords[e] for e in range(3)] + [jnp.zeros((4, SLOTS), jnp.int32)],
            axis=0,
        )
    ] + [
        part[SLOTS + QUAD :].astype(F32)[:, 0:SLOTS].astype(jnp.int32) for part in received
    ]
    quarter = iota((8, SLOTS), 1) // QUAD
    meta = jnp.zeros((8, SLOTS), jnp.int32)
    for position, part in enumerate(metas):
        moved = pltpu.roll(part, (2 * position - 3) * QUAD % SLOTS, 1)
        meta = jnp.where(quarter == position, moved, meta)
    occupied, place = meta[0:1], meta[1:4]
    half = SPAN // 2
    shifted = jnp.concatenate(
        [(place[0:1] + half) % SPAN, (place[1:2] + half) % SPAN, place[2:3]], axis=0
    )
    column = jnp.transpose(jnp.broadcast_to(occupied.astype(F32), (SLOTS, SLOTS)))
    grad = grad * jnp.concatenate([column, column], axis=1).astype(BF)
    first_weights = (w_qkv.at[0], w_out.at[0], w_up.at[0], w_down.at[0])
    second_weights = (w_qkv.at[1], w_out.at[1], w_up.at[1], w_down.at[1])
    first_out, first_saved = halo_forward(
        points, [m[1:4] for m in metas], [m[0:1] for m in metas], place, gains[0], tables[0],
        *first_weights,
    )
    hidden = first_out.astype(F32)
    second, second_saved = block_forward(
        hidden, gains[1], shifted, occupied, tables[1], *second_weights
    )
    cot, second_table = block_backward(
        grad, gains[1], shifted, second_saved, *second_weights
    )
    first_table = halo_table(cot, place, gains[0], first_saved, *first_weights[1:])
    for position, target in enumerate((own, back_y, back_x, back_xy)):
        rows = slice(position * QUAD, (position + 1) * QUAD)
        target[0:QUAD] = second[rows]
        target[QUAD:] = cot[rows]
    both = first_table + pltpu.roll(second_table, 3 * PITCH, 1)
    for i in range(tables_out.shape[0]):
        tables_out[i] = both.astype(BF)


def window_kernel(
    home_xy, home_x, home_y, own, features, occupancy, coords,
    gains, tables, w_qkv, w_out, w_up, w_down, out_points, grad_points,
):
    parts = (home_xy, home_x, home_y, own)
    second = jnp.concatenate([part[0:QUAD] for part in parts], axis=0)
    cot = jnp.concatenate([part[QUAD:] for part in parts], axis=0)
    column = jnp.transpose(jnp.broadcast_to(occupancy[...].astype(F32), (SLOTS, SLOTS)))
    out_points[...] = second * jnp.concatenate([column, column], axis=1).astype(BF)
    place = jnp.concatenate([coords[e] for e in range(3)], axis=0)
    weights = (w_qkv.at[0], w_out.at[0], w_up.at[0], w_down.at[0])
    points = features[...].astype(F32)
    _, saved = block_forward(points, gains[0], place, occupancy[...], tables[0], *weights)
    grad_points[...], _ = block_backward(
        cot, gains[0], place, saved, *weights, with_table=False
    )


def sum_of(parts):
    total = parts[0].astype(F32)
    for i in range(1, parts.shape[0]):
        total = total + parts[i].astype(F32)
    return total


def relay_kernel(parts, out):
    total = sum_of(parts).astype(BF)
    for i in range(out.shape[0]):
        out[i] = total


def unpack_kernel(parts, out):
    total = sum_of(parts)
    for k in range(2):
        for e in range(3):
            start = (3 * k + e) * PITCH
            moved = total if start == 0 else pltpu.roll(total, 128 - start, 1)
            out[k, e] = moved[:, : out.shape[-1]]


def call(kernel, shapes, *args, far=None, scratch=(), cost=None):
    options = {}
    if far is not None:
        args = args[:far] + tuple(in_hbm(a) for a in args[far:])
        options["in_specs"] = [pl.BlockSpec(memory_space=pl.ANY)] * far + [
            pl.BlockSpec(memory_space=pltpu.HBM)
        ] * (len(args) - far)
    return pl.pallas_call(
        kernel,
        out_shape=[jax.ShapeDtypeStruct(s, d) for s, d in shapes],
        scratch_shapes=scratch,
        compiler_params=pltpu.CompilerParams(vmem_limit_bytes=VMEM_LIMIT),
        cost_estimate=cost,
        interpret=INTERPRET,
        **options,
    )(*args)


def in_hbm(value):
    return value if INTERPRET else pltpu.with_memory_space_constraint(value, pltpu.HBM)


def on_device(
    gx, gy, phases,
    features, occupancy, coords, norm_gains, bias_tables, w_qkv, w_out, w_up, w_down, grad_out,
):
    size_x = lax.axis_size(gx)
    size_y = lax.axis_size(gy)

    def move(value, step_x, step_y):
        pairs = []
        for i in range(size_x):
            for j in range(size_y):
                target = (i + step_x) % size_x * size_y + (j + step_y) % size_y
                pairs.append((i * size_y + j, target))
        return lax.ppermute(value, gx + gy, pairs)

    points, occupied, grad = features[0, 0], occupancy[0], grad_out[0, 0]
    place = jnp.swapaxes(coords[0], 0, 1)
    packet, reply = ((SLOTS + QUAD + 8, WIDTH), BF), ((2 * QUAD, WIDTH), BF)
    to_y, to_x, to_xy = call(
        pack_kernel, [packet] * 3, points, occupied, place, grad, far=0,
        cost=pl.CostEstimate(flops=COST, transcendentals=0, bytes_accessed=8 * 1024 * 1024),
        scratch=[pltpu.VMEM(occupied.shape, jnp.int32), pltpu.VMEM(place.shape, jnp.int32), pltpu.SemaphoreType.DMA((8,))],
    )
    from_x = move(to_x, -1, 0)
    from_xy = move(to_xy, -1, -1)
    from_y = move(to_y, 0, -1)
    first = lax.axis_size(phases[0])
    staged = (points, occupied, place, grad, norm_gains, bias_tables, w_qkv, w_out, w_up, w_down)
    own, back_y, back_x, back_xy, tables = call(
        main_kernel,
        [reply] * 4 + [((first, HEADS, 128), BF)],
        *staged[:4], from_y, from_x, from_xy, *staged[4:],
    )
    home_y = move(back_y, 0, 1)
    home_x = move(back_x, 1, 0)
    home_xy = move(back_xy, 1, 1)
    tables = lax.all_to_all(tables, phases[0], 0, 0)
    (tables,) = call(relay_kernel, [((lax.axis_size(phases[1]), HEADS, 128), BF)], tables)
    tables = lax.all_to_all(tables, phases[1], 0, 0)
    (grad_tables,) = call(unpack_kernel, [(bias_tables.shape, F32)], tables)
    out_points, grad_points = call(
        window_kernel, [((SLOTS, WIDTH), BF)] * 2, home_xy, home_x, home_y, own, *staged[:3], *staged[4:]
    )
    return out_points[None, None], grad_points[None, None], grad_tables


def solution(mesh):
    shape = tuple(mesh.shape[a] for a in ("gx", "gy"))
    if shape == (16, 32):
        fine = Mesh(mesh.devices.reshape(2, 4, 2, 8, 4), ("zh", "y", "c", "zl", "x"))
        gx, gy = ("zh", "y", "c"), ("zl", "x")
        phases = (("zh", "zl"), ("y", "c", "x"))
    else:
        fine = Mesh(mesh.devices, ("gx", "gy"))
        gx, gy, phases = ("gx",), ("gy",), (("gx",), ("gy",))
    grid = P(gx, gy, None, None)
    return jax.shard_map(
        partial(on_device, gx, gy, phases),
        mesh=fine,
        in_specs=(grid, P(gx, gy, None), grid, P(), P(), P(), P(), P(), P(), grid),
        out_specs=(grid, grid, P()),
        check_vma=False,
    )
```
